512 devices in a mesh: groups: 2 (over y), context: 128 (over z, x), tensor: 2 (over core).
Axes of the slice: x: 8, y: 2, z: 16, core: 2. Of those that a mesh axis runs over, the one named last changes fastest.
The devices are a block of a 8x8x16 slice.
Arguments:
- self_queries: bfloat16 [20480, 2048], P(('groups', 'context'), 'tensor'), parts along dimension 0, may hold values from -512 to 512
- self_keys: bfloat16 [20480, 512], P(('groups', 'context'), 'tensor'), parts along dimension 0, may hold values from -6 to 6
- self_values: bfloat16 [20480, 512], P(('groups', 'context'), 'tensor'), parts along dimension 0, may hold values from -6 to 6
- cross_queries: bfloat16 [20480, 2048], P(('groups', 'context'), 'tensor'), parts along dimension 0, may hold values from -512 to 512
- cross_keys: bfloat16 [6144, 512], P(('groups', 'context'), 'tensor'), parts along dimension 0, may hold values from -6 to 6
- cross_values: bfloat16 [6144, 512], P(('groups', 'context'), 'tensor'), parts along dimension 0, may hold values from -6 to 6
- span_order: int32 [512], P('groups'), parts along dimension 0, may hold values from 0 to 255, as said below
Outputs:
- self_out: bfloat16 [20480, 2048], P(('groups', 'context'), 'tensor'), parts along dimension 0
- cross_out: bfloat16 [20480, 2048], P(('groups', 'context'), 'tensor'), parts along dimension 0
The draws below stay inside these ranges and needn't reach their ends.
There are 2 independent parts, one for each index of `groups`. The reference program is written for one: setup_inputs(seed, part) draws one part's arguments, and reference() takes and returns one part's arrays. A program takes and returns all parts, laid end to end along the dimension named above; each array names one. Nothing has to cross between parts.
Inputs may be any that keep to these rules, and one draw needn't show every extreme that they name: `span_order`: each of 0 to 255 appears once, and entries 2 d and 2 d + 1 sum to 255.
All inputs are finite; a program needn't handle non-finite values.
Results may differ from the reference program's by a relative error of at most 0.012.
The reference program's roundings to bfloat16 on the way count: a program that leaves them out, or rounds other values in their place, can miss the bound.
Values may be sent and summed in bfloat16 or wider, within the bound.
No kernel may reach another device: no remote copies, remote signals or barrier semaphores. Data moves between devices by JAX's collectives and lax.ppermute only.
A program may use at most 128 MiB of HBM per device.

```python
import jax
import jax.numpy as jnp
from jax import lax

HEAD_DIM = 128
HEADS = 16
KV_HEADS = 4
TEXT = 10240
IMAGE = 3072
SPAN = 40
SPANS = 256


def self_draw(key):
    key_query, key_key = jax.random.split(jax.random.fold_in(key, 17), 2)
    key_rows = jnp.clip(jax.random.normal(key_key, (TEXT, KV_HEADS, HEAD_DIM), jnp.float32), -6.0, 6.0)
    query_rows = jnp.clip(2.5 * jax.random.normal(key_query, (TEXT, HEADS, HEAD_DIM), jnp.float32), -15.0, 15.0)
    return (query_rows.reshape(TEXT, HEADS * HEAD_DIM), key_rows.reshape(TEXT, KV_HEADS * HEAD_DIM))


def cross_draw(key):
    key_query, key_key = jax.random.split(jax.random.fold_in(key, 29), 2)
    key_rows = jnp.clip(jax.random.normal(key_key, (IMAGE, KV_HEADS, HEAD_DIM), jnp.float32), -6.0, 6.0)
    query_rows = jnp.clip(2.5 * jax.random.normal(key_query, (TEXT, HEADS, HEAD_DIM), jnp.float32), -15.0, 15.0)
    return (query_rows.reshape(TEXT, HEADS * HEAD_DIM), key_rows.reshape(IMAGE, KV_HEADS * HEAD_DIM))


def draw_self_queries(key, part):
    return self_draw(key)[0].astype(jnp.bfloat16)


def draw_self_keys(key, part):
    return self_draw(key)[1].astype(jnp.bfloat16)


def draw_cross_queries(key, part):
    return cross_draw(key)[0].astype(jnp.bfloat16)


def draw_cross_keys(key, part):
    return cross_draw(key)[1].astype(jnp.bfloat16)


def draw_span_order(key, part):
    half_count = SPANS // 2
    key_owner, key_flip = jax.random.split(jax.random.fold_in(key, 5))
    owner = jax.random.permutation(key_owner, half_count).astype(jnp.int32)
    flipped = jax.random.randint(key_flip, (half_count,), 0, 2)
    late_span = SPANS - 1 - owner
    first_span = jnp.where(flipped == 1, late_span, owner)
    second_span = jnp.where(flipped == 1, owner, late_span)
    return jnp.stack([first_span, second_span], 1).reshape(-1).astype(jnp.int32)


def block_levels(own_key, dims, cuts, low, top_value):
    level = 1.0
    for position, shards_of in cuts:
        heights = jax.random.uniform(jax.random.fold_in(jax.random.fold_in(own_key, 6), position), (shards_of,), jnp.float32, low / len(cuts), top_value / len(cuts))
        level = level * jnp.repeat(jnp.exp(heights), dims[position] // shards_of).reshape((-1,) + (1,) * (len(dims) - 1 - position))
    return level


def noise(key, dims, scale, most, cuts=(), kind=jnp.bfloat16):
    array = scale * jax.random.normal(key, dims, jnp.float32)
    if cuts:
        array = array * block_levels(key, dims, cuts, -0.22, 0.18)
    return jnp.clip(array, -most, most).astype(kind)


def setup_inputs(seed: int = 0, part: int = 0) -> dict:
    arg_keys = jax.random.split(jax.random.key(seed), 8)
    own_keys = jax.random.split(jax.random.fold_in(arg_keys[7], part), 8)
    self_queries = draw_self_queries(jax.random.fold_in(jax.random.fold_in(arg_keys[7], part), 71), part)
    self_keys = draw_self_keys(jax.random.fold_in(jax.random.fold_in(arg_keys[7], part), 71), part)
    self_values = noise(own_keys[2], (TEXT, KV_HEADS * HEAD_DIM), 1.0, 6.0, ((0, 128), (1, 2)))
    cross_queries = draw_cross_queries(jax.random.fold_in(jax.random.fold_in(arg_keys[7], part), 71), part)
    cross_keys = draw_cross_keys(jax.random.fold_in(jax.random.fold_in(arg_keys[7], part), 71), part)
    cross_values = noise(own_keys[5], (IMAGE, KV_HEADS * HEAD_DIM), 1.0, 6.0, ((0, 128), (1, 2)))
    span_order = draw_span_order(jax.random.fold_in(jax.random.fold_in(arg_keys[7], part), 71), part)
    return {"self_queries": self_queries, "self_keys": self_keys, "self_values": self_values, "cross_queries": cross_queries, "cross_keys": cross_keys, "cross_values": cross_values, "span_order": span_order}


def rotary(values, places):
    half_dim = values.shape[-1] // 2
    frequency = 500000.0 ** (-(jnp.arange(half_dim, dtype=jnp.float32) * 2.0) / values.shape[-1])
    angles = places.astype(jnp.float32)[:, None] * frequency[None, :]
    cosine = jnp.cos(angles)[:, None, :]
    sine_part = jnp.sin(angles)[:, None, :]
    first_half = values[..., :half_dim]
    second_half = values[..., half_dim:]
    return jnp.concatenate([first_half * cosine - second_half * sine_part, second_half * cosine + first_half * sine_part], -1)


def attend_block(queries, key_rows, value_rows, query_places, key_places):
    scores = jnp.einsum("qkgd,rkd->kgqr", queries.astype(jnp.float32), key_rows.astype(jnp.float32)) * (HEAD_DIM ** -0.5)
    if key_places is not None:
        allowed = key_places[None, :] <= query_places[:, None]
        scores = jnp.where(allowed[None, None], scores, -jnp.inf)
    row_peak = jnp.max(scores, -1, keepdims=True)
    weights = jnp.exp(scores - row_peak)
    weight_sum = jnp.sum(weights, -1)
    rounded = lax.optimization_barrier(weights.astype(jnp.bfloat16))
    mixed_sum = jnp.einsum("kgqr,rkd->qkgd", rounded.astype(jnp.float32), value_rows.astype(jnp.float32))
    return mixed_sum / jnp.transpose(weight_sum, (2, 0, 1))[..., None]


def attention(queries, key_rows, value_rows, query_places, key_places):
    row_total = queries.shape[0]
    block_rows = min(512, row_total)
    while row_total % block_rows != 0:
        block_rows = block_rows // 2
    query_blocks = queries.reshape((row_total // block_rows, block_rows) + queries.shape[1:])
    if key_places is None:
        def per_block(query_block):
            return attend_block(query_block, key_rows, value_rows, None, None)
        result = lax.map(per_block, query_blocks)
    else:
        place_blocks = query_places.reshape(row_total // block_rows, block_rows)

        def per_masked(arrived):
            return attend_block(arrived[0], key_rows, value_rows, arrived[1], key_places)
        result = lax.map(per_masked, (query_blocks, place_blocks))
    return result.reshape(row_total, -1).astype(jnp.bfloat16)


def reference(self_queries, self_keys, self_values, cross_queries, cross_keys, cross_values, span_order):
    group_size = HEADS // KV_HEADS
    places = (span_order[:, None] * SPAN + jnp.arange(SPAN, dtype=jnp.int32)[None, :]).reshape(-1).astype(jnp.int32)
    text_queries = rotary(self_queries.astype(jnp.float32).reshape(TEXT, HEADS, HEAD_DIM), places).astype(jnp.bfloat16)
    text_queries = lax.optimization_barrier(text_queries).reshape(TEXT, KV_HEADS, group_size, HEAD_DIM)
    text_keys = rotary(self_keys.astype(jnp.float32).reshape(TEXT, KV_HEADS, HEAD_DIM), places).astype(jnp.bfloat16)
    text_keys = lax.optimization_barrier(text_keys)
    self_out = attention(text_queries, text_keys, self_values.reshape(TEXT, KV_HEADS, HEAD_DIM), places, places)
    image_queries = cross_queries.reshape(TEXT, KV_HEADS, group_size, HEAD_DIM)
    cross_out = attention(image_queries, cross_keys.reshape(IMAGE, KV_HEADS, HEAD_DIM), cross_values.reshape(IMAGE, KV_HEADS, HEAD_DIM), None, None)
    return (self_out, cross_out)
```

```python
import jax
import jax.numpy as jnp
import numpy as np
from jax import lax
from jax.experimental import pallas as pl
from jax.experimental.pallas import tpu as pltpu
from jax.sharding import PartitionSpec as P

HEAD_DIM = 128
HEADS = 16
KV_HEADS = 4
GROUP = HEADS // KV_HEADS
RING = 8
STEP_DEVICES = 4
NEG_FILL = -1e30
LOG2E = 1.4426950408889634

BF16 = jnp.bfloat16
F32 = jnp.float32


def rows_of(*pieces):
    return jnp.concatenate(pieces, 0)


def frequencies():
    lane = np.arange(HEAD_DIM) % (HEAD_DIM // 2)
    return (500000.0 ** (-(lane * 2.0) / HEAD_DIM)).astype(np.float32)[None, :]


def prepare_kernel(order, freq, sq, sk, sv, cq, ck, cv, q_out, kv_out):
    me = lax.axis_index("context")
    rows = sq.shape[0]
    span = rows // 2
    first, second = order[2 * me], order[2 * me + 1]
    swap = first > second
    early, late = jnp.minimum(first, second), jnp.maximum(first, second)
    row = lax.broadcasted_iota(jnp.int32, (rows, HEAD_DIM), 0)
    lane = lax.broadcasted_iota(jnp.int32, (rows, HEAD_DIM), 1)
    place = jnp.where(row < span, early * span + row, late * span + row - span)
    angle = place.astype(F32) * freq[...]
    cosine = jnp.cos(angle)
    sine = jnp.sin(angle)
    sine = jnp.where(lane < HEAD_DIM // 2, -sine, sine)

    def ordered(ref, head):
        x = ref[:, head * HEAD_DIM : (head + 1) * HEAD_DIM].astype(F32)
        return jnp.where(swap, rows_of(x[span:], x[:span]), x)

    def rotated(ref, head):
        x = ordered(ref, head)
        return x * cosine + pltpu.roll(x, HEAD_DIM // 2, 1) * sine

    def plain(ref, head):
        return ref[:, head * HEAD_DIM : (head + 1) * HEAD_DIM].astype(F32)

    heads = sq.shape[1] // HEAD_DIM
    copies = q_out.shape[0] // heads
    for head in range(heads):
        block = rows_of(rotated(sq, head), plain(cq, head)).astype(BF16)
        for c in range(copies):
            q_out[head * copies + c] = block
    for kv in range(heads // GROUP):
        block = rows_of(
            rotated(sk, kv), ordered(sv, kv), plain(ck, kv), plain(cv, kv)
        ).astype(BF16)
        for g in range(GROUP):
            kv_out[kv * GROUP + g] = block


def attend_kernel(
    subsets, order, q_in, kv_in, out, key_e, key_l, val_e, val_l, key_c, val_c, pos_e, pos_l
):
    step = pl.program_id(0)
    me = lax.axis_index("context")
    column = me % RING
    subset = (me // RING) % subsets
    rows = q_in.shape[1] // 2
    span = rows // 2
    image = kv_in.shape[1] // 2 - rows
    key_devices = kv_in.shape[0]
    per_column = key_devices // RING

    def spans_of(device):
        first, second = order[2 * device], order[2 * device + 1]
        return jnp.minimum(first, second), jnp.maximum(first, second)

    @pl.when(step == 0)
    def _():
        def pair(i, carry):
            a = kv_in[2 * i].astype(F32)
            b = kv_in[2 * i + 1].astype(F32)

            def put(ref, lo, hi):
                size = 2 * (hi - lo)
                at = pl.multiple_of(i * size, size)
                ref[pl.ds(at, size), :] = rows_of(a[lo:hi], b[lo:hi]).astype(BF16)

            put(key_e, 0, span)
            put(key_l, span, rows)
            put(val_e, rows, rows + span)
            put(val_l, rows + span, 2 * rows)
            put(key_c, 2 * rows, 2 * rows + image)
            put(val_c, 2 * rows + image, 2 * rows + 2 * image)
            return carry

        lax.fori_loop(0, key_devices // 2, pair, 0)
        lane = lax.broadcasted_iota(jnp.int32, pos_e.shape, 1)
        place_e, place_l = lane, lane
        for d in range(key_devices):
            device = ((d % per_column) * subsets + subset) * RING + d // per_column
            early, late = spans_of(device)
            here = lane >= d * span
            place_e = jnp.where(here, lane + (early - d) * span, place_e)
            place_l = jnp.where(here, lane + (late - d) * span, place_l)
        pos_e[...] = place_e
        pos_l[...] = place_l

    scale = HEAD_DIM ** (-0.5) * LOG2E
    blocks = [q_in[i].astype(F32) for i in range(STEP_DEVICES)]
    q_e = rows_of(*[b[:span] for b in blocks]).astype(BF16)
    q_l = rows_of(*[b[span:rows] for b in blocks]).astype(BF16)
    q_c = rows_of(*[b[rows:] for b in blocks]).astype(BF16)
    size = STEP_DEVICES * span
    row = lax.broadcasted_iota(jnp.int32, (size, 1), 0)
    place_e, place_l = row, row
    for i in range(STEP_DEVICES):
        early, late = spans_of((step * STEP_DEVICES + i) * RING + column)
        here = row >= i * span
        place_e = jnp.where(here, row + (early - i) * span, place_e)
        place_l = jnp.where(here, row + (late - i) * span, place_l)

    def scores(q, key):
        return lax.dot_general(
            q, key[...], (((1,), (1,)), ((), ())), preferred_element_type=F32
        )

    def finish(parts):
        peak = parts[0][0].max(-1, keepdims=True)
        for s, _ in parts[1:]:
            peak = jnp.maximum(peak, s.max(-1, keepdims=True))
        shift = jnp.maximum(peak, 0.1 * NEG_FILL)
        total, mixed = 0.0, 0.0
        for s, val in parts:
            w = jnp.exp2((s - shift) * scale)
            total = total + w.sum(-1, keepdims=True)
            mixed = mixed + jnp.dot(w.astype(BF16), val[...], preferred_element_type=F32)
        some = total > 0.0
        safe = jnp.where(some, total, 1.0)
        level = jnp.where(some, shift * scale + jnp.log2(safe), NEG_FILL)
        return mixed / safe, level

    def masked(s, key_places, query_places):
        return jnp.where(key_places[...] <= query_places, s, NEG_FILL)

    out_l, level_l = finish(
        [
            (scores(q_l, key_e), val_e),
            (masked(scores(q_l, key_l), pos_l, place_l), val_l),
        ]
    )
    out_e, level_e = finish([(masked(scores(q_e, key_e), pos_e, place_e), val_e)])
    out_c, level_c = finish([(scores(q_c, key_c), val_c)])

    lane = lax.broadcasted_iota(jnp.int32, (HEAD_DIM, HEAD_DIM), 1)
    for i in range(STEP_DEVICES):

        def mine(a, n):
            return a[i * n : (i + 1) * n]

        level = rows_of(mine(level_e, span), mine(level_l, span), mine(level_c, rows))
        table = jnp.zeros((HEAD_DIM, HEAD_DIM), F32)
        for c, chunk in enumerate((level[:HEAD_DIM], level[2 * rows - HEAD_DIM :])):
            for piece in range(3):
                part = chunk.astype(BF16).astype(F32)
                table = jnp.where(lane == 3 * c + piece, part, table)
                chunk = chunk - part
        out[i] = rows_of(
            mine(out_e, span), mine(out_l, span), mine(out_c, rows), table.T[:8]
        ).astype(BF16)


def combine_kernel(subsets, order, parts, self_out, cross_out):
    me = lax.axis_index("context")
    rows = self_out.shape[0]
    span = rows // 2
    swap = order[2 * me] > order[2 * me + 1]
    heads = parts.shape[0] // subsets
    levels = []
    for s in range(parts.shape[0]):
        t = parts[s, 2 * rows : 2 * rows + 8, :].astype(F32)
        levels.append((t[0:1] + t[1:2] + t[2:3], t[3:4] + t[4:5] + t[5:6]))
    shares = [[], []]
    for head in range(heads):
        for c in range(2):
            own = [levels[head * subsets + p][c] for p in range(subsets)]
            peak = own[0]
            for level in own[1:]:
                peak = jnp.maximum(peak, level)
            weights = [jnp.exp2(level - peak) for level in own]
            total = weights[0]
            for w in weights[1:]:
                total = total + w
            shares[c] += [w / total for w in weights]
    count = 2 * parts.shape[0]
    table = rows_of(*shares[0], *shares[1], jnp.zeros((HEAD_DIM - count, HEAD_DIM), F32)).T
    for head in range(heads):
        mixed = 0.0
        for p in range(subsets):
            s = head * subsets + p
            again = 2 * HEAD_DIM - 2 * rows
            other = parts.shape[0] + s
            share = rows_of(table[:, s : s + 1], table[again:, other : other + 1])
            mixed = mixed + share * parts[s, : 2 * rows, :].astype(F32)
        columns = slice(head * HEAD_DIM, (head + 1) * HEAD_DIM)
        first, second = mixed[:span], mixed[span:rows]
        self_out[:, columns] = jnp.where(
            swap, rows_of(second, first), rows_of(first, second)
        ).astype(BF16)
        cross_out[:, columns] = mixed[rows:].astype(BF16)


def whole(memory=pltpu.VMEM):
    return pl.BlockSpec(memory_space=memory)


def body(self_queries, self_keys, self_values, cross_queries, cross_keys, cross_values, span_order):
    context = lax.axis_size("context")
    rows = self_queries.shape[0]
    image = cross_keys.shape[0]
    heads = self_queries.shape[1] // HEAD_DIM
    height = context // RING
    subsets = height // heads
    columns = [[z * RING + x for z in range(height)] for x in range(RING)]
    subset_columns = [c[p::subsets] for c in columns for p in range(subsets)]
    lines = [[z * RING + x for x in range(RING)] for z in range(height)]
    key_devices = RING * heads
    kv_rows = 2 * (rows + image)

    queries, keys = pl.pallas_call(
        prepare_kernel,
        in_specs=[whole(pltpu.SMEM)] + [whole()] * 7,
        out_specs=[whole(), whole()],
        out_shape=[
            jax.ShapeDtypeStruct((height, 2 * rows, HEAD_DIM), BF16),
            jax.ShapeDtypeStruct((heads, kv_rows, HEAD_DIM), BF16),
        ],
        name="prepare",
    )(
        span_order,
        jnp.asarray(frequencies()),
        self_queries,
        self_keys,
        self_values,
        cross_queries,
        cross_keys,
        cross_values,
    )
    keys = lax.all_to_all(keys, "context", 0, 0, axis_index_groups=subset_columns)
    keys = lax.all_gather(keys, "context", axis_index_groups=lines)
    queries = lax.all_to_all(queries, "context", 0, 0, axis_index_groups=columns)

    out_rows = 2 * rows + 8
    span_keys = key_devices * rows // 2
    partial_out = pl.pallas_call(
        lambda *refs: attend_kernel(subsets, *refs),
        grid=(height // STEP_DEVICES,),
        in_specs=[
            whole(pltpu.SMEM),
            pl.BlockSpec((STEP_DEVICES, 2 * rows, HEAD_DIM), lambda i: (i, 0, 0)),
            pl.BlockSpec((key_devices, kv_rows, HEAD_DIM), lambda i: (0, 0, 0)),
        ],
        out_specs=pl.BlockSpec((STEP_DEVICES, out_rows, HEAD_DIM), lambda i: (i, 0, 0)),
        out_shape=jax.ShapeDtypeStruct((height, out_rows, HEAD_DIM), BF16),
        scratch_shapes=[pltpu.VMEM((span_keys, HEAD_DIM), BF16)] * 4
        + [pltpu.VMEM((key_devices * image, HEAD_DIM), BF16)] * 2
        + [pltpu.VMEM((1, span_keys), jnp.int32)] * 2,
        compiler_params=pltpu.CompilerParams(
            dimension_semantics=("arbitrary",), vmem_limit_bytes=56 * 1024 * 1024
        ),
        name="attend",
    )(span_order, queries, keys.reshape(key_devices, kv_rows, HEAD_DIM))
    partial_out = lax.all_to_all(partial_out, "context", 0, 0, axis_index_groups=columns)

    return tuple(
        pl.pallas_call(
            lambda *refs: combine_kernel(subsets, *refs),
            in_specs=[whole(pltpu.SMEM), whole()],
            out_specs=[whole(), whole()],
            out_shape=[jax.ShapeDtypeStruct((rows, heads * HEAD_DIM), BF16)] * 2,
            name="combine",
        )(span_order, partial_out)
    )


def solution(mesh):
    rows = P(("groups", "context"), "tensor")
    return jax.shard_map(
        body,
        mesh=mesh,
        in_specs=(rows,) * 6 + (P("groups"),),
        out_specs=(rows, rows),
        check_vma=False,
    )
```

```python
import jax
import jax.numpy as jnp
import numpy as np
from jax import lax
from jax.experimental import pallas as pl
from jax.experimental.pallas import tpu as pltpu
from jax.sharding import PartitionSpec as P

HEAD_DIM = 128
HEADS = 16
KV_HEADS = 4
GROUP = HEADS // KV_HEADS
RING = 8
PAIR = 2
PIECES = 3
NEG_FILL = -1e30
LOG2E = 1.4426950408889634

BF16 = jnp.bfloat16
F32 = jnp.float32


def rows_of(*pieces):
    return jnp.concatenate(pieces, 0)


def frequencies():
    lane = np.arange(HEAD_DIM) % (HEAD_DIM // 2)
    return (500000.0 ** (-(lane * 2.0) / HEAD_DIM)).astype(np.float32)[None, :]


def prepare_kernel(order, freq, sq, sk, sv, cq, ck, cv, q_out, kv_out):
    me = lax.axis_index("context")
    rows = sq.shape[0]
    span = rows // 2
    first, second = order[2 * me], order[2 * me + 1]
    swap = first > second
    early, late = jnp.minimum(first, second), jnp.maximum(first, second)
    row = lax.broadcasted_iota(jnp.int32, (rows, HEAD_DIM), 0)
    lane = lax.broadcasted_iota(jnp.int32, (rows, HEAD_DIM), 1)
    place = jnp.where(row < span, early * span + row, late * span + row - span)
    angle = place.astype(F32) * freq[...]
    cosine = jnp.cos(angle)
    sine = jnp.sin(angle)
    sine = jnp.where(lane < HEAD_DIM // 2, -sine, sine)

    def ordered(ref, head):
        x = ref[:, head * HEAD_DIM : (head + 1) * HEAD_DIM].astype(F32)
        return jnp.where(swap, rows_of(x[span:], x[:span]), x)

    def rotated(ref, head):
        x = ordered(ref, head)
        return x * cosine + pltpu.roll(x, HEAD_DIM // 2, 1) * sine

    def plain(ref, head):
        return ref[:, head * HEAD_DIM : (head + 1) * HEAD_DIM].astype(F32)

    kv_local = sk.shape[1] // HEAD_DIM
    for kv in range(kv_local):
        block = rows_of(
            rotated(sk, kv), ordered(sv, kv), plain(ck, kv), plain(cv, kv)
        ).astype(BF16)
        for m in range(kv, kv_out.shape[0], kv_local):
            kv_out[m] = block
    for kv in range(kv_local):
        heads = range(kv * GROUP, (kv + 1) * GROUP)
        turned = [rotated(sq, head) for head in heads]
        block = rows_of(
            *[x[:span] for x in turned],
            *[x[span:] for x in turned],
            *[plain(cq, head) for head in heads],
        ).astype(BF16)
        for m in range(kv, q_out.shape[0], kv_local):
            q_out[m] = block


def spans_of(order, device):
    first, second = order[2 * device], order[2 * device + 1]
    return jnp.minimum(first, second), jnp.maximum(first, second)


def scores(q, key):
    return lax.dot_general(q, key[...], (((1,), (1,)), ((), ())), preferred_element_type=F32)


def finish(parts):
    scale = HEAD_DIM ** (-0.5) * LOG2E
    peak = parts[0][0].max(-1, keepdims=True)
    for s, _ in parts[1:]:
        peak = jnp.maximum(peak, s.max(-1, keepdims=True))
    shift = jnp.maximum(peak, 0.1 * NEG_FILL)
    total, mixed = 0.0, 0.0
    for s, val in parts:
        w = jnp.exp2((s - shift) * scale)
        total = total + w.sum(-1, keepdims=True)
        mixed = mixed + jnp.dot(w.astype(BF16), val[...], preferred_element_type=F32)
    some = total > 0.0
    safe = jnp.where(some, total, 1.0)
    level = jnp.where(some, shift * scale + jnp.log2(safe), NEG_FILL)
    return mixed / safe, level


def chunks_of(size):
    return [min(at, size - HEAD_DIM) for at in range(0, size, HEAD_DIM)]


def stat_rows(size):
    return -(-PIECES * len(chunks_of(size)) // 16) * 16


def with_levels(mixed, level):
    lane = lax.broadcasted_iota(jnp.int32, (HEAD_DIM, HEAD_DIM), 1)
    table = jnp.zeros((HEAD_DIM, HEAD_DIM), F32)
    for c, at in enumerate(chunks_of(level.shape[0])):
        rest = level[at : at + HEAD_DIM]
        for piece in range(PIECES):
            part = rest.astype(BF16).astype(F32)
            table = jnp.where(lane == PIECES * c + piece, part, table)
            rest = rest - part
    return rows_of(mixed, table.T[: stat_rows(level.shape[0])]).astype(BF16)


def gathered_rows(kv_in, targets):
    def pair(i, carry):
        a = kv_in[2 * i].astype(F32)
        b = kv_in[2 * i + 1].astype(F32)
        for ref, lo, hi in targets:
            size = 2 * (hi - lo)
            at = pl.multiple_of(i * size, size)
            ref[pl.ds(at, size), :] = rows_of(a[lo:hi], b[lo:hi]).astype(BF16)
        return carry

    lax.fori_loop(0, kv_in.shape[0] // 2, pair, 0)


def cross_kernel(rows, q_in, kv_in, out, key, val):
    image = kv_in.shape[1] // 2 - rows

    @pl.when(pl.program_id(0) == 0)
    def _():
        low = 2 * rows
        gathered_rows(kv_in, [(key, low, low + image), (val, low + image, low + 2 * image)])

    out[0] = with_levels(*finish([(scores(q_in[0], key), val)]))


def self_kernel(rows, order, q_in, kv_in, out, key_e, key_l, val_e, val_l, pos_e, pos_l):
    step = pl.program_id(0)
    me = lax.axis_index("context")
    span = rows // 2

    @pl.when(step == 0)
    def _():
        gathered_rows(
            kv_in,
            [
                (key_e, 0, span),
                (key_l, span, rows),
                (val_e, rows, rows + span),
                (val_l, rows + span, 2 * rows),
            ],
        )
        pair = me % RING // PAIR
        lane = lax.broadcasted_iota(jnp.int32, pos_e.shape, 1)
        place_e, place_l = lane, lane
        for d in range(kv_in.shape[0]):
            line, column = d // PAIR, pair * PAIR + d % PAIR
            early, late = spans_of(order, line * RING + column)
            here = lane >= d * span
            place_e = jnp.where(here, lane + (early - d) * span, place_e)
            place_l = jnp.where(here, lane + (late - d) * span, place_l)
        pos_e[...] = place_e
        pos_l[...] = place_l

    size = GROUP * span
    early, late = spans_of(order, me // RING * RING + step)
    within = lax.broadcasted_iota(jnp.int32, (size, 1), 0) % span

    def masked(s, key_places, query_places):
        return jnp.where(key_places[...] <= query_places, s, NEG_FILL)

    q_e, q_l = q_in[0, :size], q_in[0, size:]
    out_e, level_e = finish([(masked(scores(q_e, key_e), pos_e, early * span + within), val_e)])
    out_l, level_l = finish(
        [
            (scores(q_l, key_e), val_e),
            (masked(scores(q_l, key_l), pos_l, late * span + within), val_l),
        ]
    )
    out[0] = with_levels(rows_of(out_e, out_l), rows_of(level_e, level_l))


def combine_kernel(order, self_parts, cross_parts, self_out, cross_out):
    me = lax.axis_index("context")
    rows = self_out.shape[0]
    span = rows // 2
    swap = order[2 * me] > order[2 * me + 1]
    kv_local = self_out.shape[1] // (HEAD_DIM * GROUP)
    subsets = self_parts.shape[0] // kv_local
    size = GROUP * rows
    starts = chunks_of(size)

    def mix(parts):
        shares = [[None] * len(starts) for _ in range(parts.shape[0])]
        for kv in range(kv_local):
            members = [j * kv_local + kv for j in range(subsets)]
            stats = [parts[s, size:, :].astype(F32) for s in members]
            for c in range(len(starts)):
                own = []
                for t in stats:
                    level = t[PIECES * c : PIECES * c + 1]
                    for piece in range(1, PIECES):
                        level = level + t[PIECES * c + piece : PIECES * c + piece + 1]
                    own.append(level)
                peak = own[0]
                for level in own[1:]:
                    peak = jnp.maximum(peak, level)
                weights = [jnp.exp2(level - peak) for level in own]
                total = weights[0]
                for w in weights[1:]:
                    total = total + w
                for s, w in zip(members, weights):
                    shares[s][c] = w / total
        flat = [w for share in shares for w in share]
        table = rows_of(*flat, jnp.zeros((HEAD_DIM - len(flat), HEAD_DIM), F32)).T
        results = []
        for kv in range(kv_local):
            mixed = 0.0
            for j in range(subsets):
                s = j * kv_local + kv
                pieces, done = [], 0
                for c, at in enumerate(starts):
                    column = s * len(starts) + c
                    pieces.append(table[done - at :, column : column + 1])
                    done = at + HEAD_DIM
                mixed = mixed + rows_of(*pieces) * parts[s, :size, :].astype(F32)
            results.append(mixed)
        return results

    for kv, mixed in enumerate(mix(self_parts)):
        for g in range(GROUP):
            head = kv * GROUP + g
            early = mixed[g * span : (g + 1) * span]
            late = mixed[(GROUP + g) * span : (GROUP + g + 1) * span]
            self_out[:, head * HEAD_DIM : (head + 1) * HEAD_DIM] = jnp.where(
                swap, rows_of(late, early), rows_of(early, late)
            ).astype(BF16)
    for kv, mixed in enumerate(mix(cross_parts)):
        for g in range(GROUP):
            head = kv * GROUP + g
            cross_out[:, head * HEAD_DIM : (head + 1) * HEAD_DIM] = mixed[
                g * rows : (g + 1) * rows
            ].astype(BF16)


def whole(memory=pltpu.VMEM):
    return pl.BlockSpec(memory_space=memory)


def body(self_queries, self_keys, self_values, cross_queries, cross_keys, cross_values, span_order):
    context = lax.axis_size("context")
    rows = self_queries.shape[0]
    image = cross_keys.shape[0]
    heads = self_queries.shape[1] // HEAD_DIM
    height = context // RING
    lines = [[z * RING + x for x in range(RING)] for z in range(height)]
    squares = [
        [(z + a) * RING + x + b for a in range(PAIR) for b in range(PAIR)]
        for z in range(0, height, PAIR)
        for x in range(0, RING, PAIR)
    ]
    columns = [
        [z * RING + x for z in range(p, height, PAIR)] for p in range(PAIR) for x in range(RING)
    ]
    key_devices = height * PAIR
    kv_rows = 2 * (rows + image)
    size = GROUP * rows

    queries, keys = pl.pallas_call(
        prepare_kernel,
        in_specs=[whole(pltpu.SMEM)] + [whole()] * 7,
        out_specs=[whole(), whole()],
        out_shape=[
            jax.ShapeDtypeStruct((RING, 2 * size, HEAD_DIM), BF16),
            jax.ShapeDtypeStruct((PAIR * PAIR, kv_rows, HEAD_DIM), BF16),
        ],
        name="prepare",
    )(
        span_order,
        jnp.asarray(frequencies()),
        self_queries,
        self_keys,
        self_values,
        cross_queries,
        cross_keys,
        cross_values,
    )
    keys = lax.all_to_all(keys, "context", 0, 0, axis_index_groups=squares)
    keys = lax.all_gather(keys, "context", axis_index_groups=columns)
    queries = lax.all_to_all(queries, "context", 0, 0, axis_index_groups=lines)
    keys = keys.reshape(key_devices, kv_rows, HEAD_DIM)

    out_rows = size + stat_rows(size)

    def attend(kernel, half, order, scratch, name):
        return pl.pallas_call(
            lambda *refs: kernel(rows, *refs),
            grid=(RING,),
            in_specs=[whole(pltpu.SMEM)] * len(order)
            + [
                pl.BlockSpec((1, size, HEAD_DIM), lambda i: (i, half, 0)),
                pl.BlockSpec((key_devices, kv_rows, HEAD_DIM), lambda i: (0, 0, 0)),
            ],
            out_specs=pl.BlockSpec((1, out_rows, HEAD_DIM), lambda i: (i, 0, 0)),
            out_shape=jax.ShapeDtypeStruct((RING, out_rows, HEAD_DIM), BF16),
            scratch_shapes=scratch,
            compiler_params=pltpu.CompilerParams(
                dimension_semantics=("arbitrary",), vmem_limit_bytes=48 * 1024 * 1024
            ),
            cost_estimate=pl.CostEstimate(
                flops=4 * RING * size * HEAD_DIM * key_devices * rows,
                transcendentals=RING * size * key_devices * rows,
                bytes_accessed=2 * key_devices * kv_rows * HEAD_DIM,
            ),
            name=name,
        )(*order, queries, keys)

    span_keys = key_devices * rows // 2
    image_keys = key_devices * image
    cross_parts = attend(
        cross_kernel, 1, (), [pltpu.VMEM((image_keys, HEAD_DIM), BF16)] * 2, "cross"
    )
    cross_parts = lax.all_to_all(cross_parts, "context", 0, 0, axis_index_groups=lines)
    self_parts = attend(
        self_kernel,
        0,
        (span_order,),
        [pltpu.VMEM((span_keys, HEAD_DIM), BF16)] * 4 + [pltpu.VMEM((1, span_keys), jnp.int32)] * 2,
        "self",
    )
    self_parts = lax.all_to_all(self_parts, "context", 0, 0, axis_index_groups=lines)

    return tuple(
        pl.pallas_call(
            combine_kernel,
            in_specs=[whole(pltpu.SMEM), whole(), whole()],
            out_specs=[whole(), whole()],
            out_shape=[jax.ShapeDtypeStruct((rows, heads * HEAD_DIM), BF16)] * 2,
            name="combine",
        )(span_order, self_parts, cross_parts)
    )


def solution(mesh):
    rows = P(("groups", "context"), "tensor")
    return jax.shard_map(
        body,
        mesh=mesh,
        in_specs=(rows,) * 6 + (P("groups"),),
        out_specs=(rows, rows),
        check_vma=False,
    )
```

```python
import jax
import jax.numpy as jnp
import numpy as np
from jax import lax
from jax.experimental import pallas as pl
from jax.experimental.pallas import tpu as pltpu
from jax.sharding import PartitionSpec as P


HEAD_DIM = 128
HEADS = 16
KV_HEADS = 4
GROUP = HEADS // KV_HEADS
RING = 8
HALF = RING // 2
PAIR = 2
STEP = 4
PIECES = 3
NEG_FILL = -1e30
LOG2E = 1.4426950408889634

BF16 = jnp.bfloat16
F32 = jnp.float32


def rows_of(*pieces):
    return jnp.concatenate(pieces, 0)


def frequencies():
    lane = np.arange(HEAD_DIM) % (HEAD_DIM // 2)
    return (500000.0 ** (-(lane * 2.0) / HEAD_DIM)).astype(np.float32)[None, :]


def spans_of(order, device):
    first, second = order[2 * device], order[2 * device + 1]
    return jnp.minimum(first, second), jnp.maximum(first, second)


def local_order(order, freq, rows):
    me = lax.axis_index("context")
    span = rows // 2
    swap = order[2 * me] > order[2 * me + 1]
    early, late = spans_of(order, me)
    row = lax.broadcasted_iota(jnp.int32, (rows, HEAD_DIM), 0)
    lane = lax.broadcasted_iota(jnp.int32, (rows, HEAD_DIM), 1)
    place = jnp.where(row < span, early * span + row, late * span + row - span)
    angle = place.astype(F32) * freq[...]
    cosine = jnp.cos(angle)
    sine = jnp.sin(angle)
    sine = jnp.where(lane < HEAD_DIM // 2, -sine, sine)

    def ordered(ref, head):
        x = plain(ref, head)
        return jnp.where(swap, rows_of(x[span:], x[:span]), x)

    def rotated(ref, head):
        x = ordered(ref, head)
        return x * cosine + pltpu.roll(x, HEAD_DIM // 2, 1) * sine

    return ordered, rotated


def plain(ref, head):
    return ref[:, head * HEAD_DIM : (head + 1) * HEAD_DIM].astype(F32)


def prepare_kernel(order, freq, sq, sk, sv, cq, ck, cv, q_out, kv_out):
    rows = sq.shape[0]
    span = rows // 2
    ordered, rotated = local_order(order, freq, rows)
    kv_local = sk.shape[1] // HEAD_DIM
    for kv in range(kv_local):
        block = rows_of(
            rotated(sk, kv), ordered(sv, kv), plain(ck, kv), plain(cv, kv)
        ).astype(BF16)
        for m in range(kv, kv_out.shape[0], kv_local):
            kv_out[m] = block
    for kv in range(kv_local):
        heads = range(kv * GROUP, (kv + 1) * GROUP)
        turned = [rotated(sq, head) for head in heads]
        block = rows_of(
            *[x[:span] for x in turned],
            *[x[span:] for x in turned],
            *[plain(cq, head) for head in heads],
        ).astype(BF16)
        for m in range(kv, q_out.shape[0], kv_local):
            q_out[m] = block


def scores(q, key):
    return lax.dot_general(q, key[...], (((1,), (1,)), ((), ())), preferred_element_type=F32)


def peak_of(parts):
    peak = parts[0].max(-1, keepdims=True)
    for s in parts[1:]:
        peak = jnp.maximum(peak, s.max(-1, keepdims=True))
    return jnp.maximum(peak, 0.1 * NEG_FILL)


def finish(parts):
    scale = HEAD_DIM ** (-0.5) * LOG2E
    shift = peak_of([s for s, _ in parts])
    total, mixed = 0.0, 0.0
    for s, val in parts:
        w = jnp.exp2((s - shift) * scale)
        total = total + w.sum(-1, keepdims=True)
        mixed = mixed + jnp.dot(w.astype(BF16), val[...], preferred_element_type=F32)
    some = total > 0.0
    safe = jnp.where(some, total, 1.0)
    level = jnp.where(some, shift * scale + jnp.log2(safe), NEG_FILL)
    return mixed * (1.0 / safe), level


def chunks_of(size):
    return [min(at, size - HEAD_DIM) for at in range(0, size, HEAD_DIM)]


def stat_rows(size):
    return -(-PIECES * len(chunks_of(size)) // 16) * 16


def with_levels(mixed, level):
    lane = lax.broadcasted_iota(jnp.int32, (HEAD_DIM, HEAD_DIM), 1)
    table = jnp.zeros((HEAD_DIM, HEAD_DIM), F32)
    for c, at in enumerate(chunks_of(level.shape[0])):
        rest = level[at : at + HEAD_DIM]
        for piece in range(PIECES):
            part = rest.astype(BF16).astype(F32)
            table = jnp.where(lane == PIECES * c + piece, part, table)
            rest = rest - part
    return rows_of(mixed, table.T[: stat_rows(level.shape[0])]).astype(BF16)


def gathered_rows(kv_in, targets):
    def pair(i, carry):
        a = kv_in[2 * i].astype(F32)
        b = kv_in[2 * i + 1].astype(F32)
        for ref, lo, hi in targets:
            size = 2 * (hi - lo)
            at = pl.multiple_of(i * size, size)
            ref[pl.ds(at, size), :] = rows_of(a[lo:hi], b[lo:hi]).astype(BF16)
        return carry

    lax.fori_loop(0, kv_in.shape[0] // 2, pair, 0)


def cross_kernel(rows, q_in, kv_hbm, out, kv_in, key, val, sem):
    image = kv_in.shape[1] // 2

    @pl.when(pl.program_id(0) == 0)
    def _():
        copy = pltpu.make_async_copy(kv_hbm.at[:, 2 * rows : 2 * rows + 2 * image, :], kv_in, sem)
        copy.start()
        copy.wait()
        gathered_rows(kv_in, [(key, 0, image), (val, image, 2 * image)])

    s = [scores(q_in[i], key) for i in range(STEP)]
    for i in range(STEP):
        out[i] = with_levels(*finish([(s[i], val)]))


def self_kernel(rows, order, q_in, kv_in, out, key_e, key_l, val_e, val_l, pos_e, pos_l):
    step = pl.program_id(0)
    me = lax.axis_index("context")
    line, column = me // RING, me % RING
    span = rows // 2

    @pl.when(step == 0)
    def _():
        gathered_rows(
            kv_in,
            [
                (key_e, 0, span),
                (key_l, span, rows),
                (val_e, rows, rows + span),
                (val_l, rows + span, 2 * rows),
            ],
        )
        low = line % PAIR * RING + column % HALF // PAIR * PAIR
        lane = lax.broadcasted_iota(jnp.int32, pos_e.shape, 1)
        place_e, place_l = lane, lane
        for d in range(kv_in.shape[0]):
            b = d % (PAIR * PAIR)
            device = low + d // (PAIR * PAIR) * PAIR * RING + b // PAIR * HALF + b % PAIR
            early, late = spans_of(order, device)
            here = lane >= d * span
            place_e = jnp.where(here, lane + (early - d) * span, place_e)
            place_l = jnp.where(here, lane + (late - d) * span, place_l)
        pos_e[...] = place_e
        pos_l[...] = place_l

    size = GROUP * span
    within = lax.broadcasted_iota(jnp.int32, (size, 1), 0) % span
    base = line // PAIR * PAIR * RING + column // HALF * HALF

    def masked(s, key_places, query_places):
        return jnp.where(key_places[...] <= query_places, s, NEG_FILL)

    s_ee, s_le, s_ll, ends = [], [], [], []
    for i in range(STEP):
        source = step * STEP + i
        ends.append(spans_of(order, base + source // HALF * RING + source % HALF))
        q_e, q_l = q_in[i, :size], q_in[i, size:]
        s_ee.append(scores(q_e, key_e))
        s_le.append(scores(q_l, key_e))
        s_ll.append(scores(q_l, key_l))
    for i in range(STEP):
        early, late = ends[i]
        out_e, level_e = finish([(masked(s_ee[i], pos_e, early * span + within), val_e)])
        out_l, level_l = finish(
            [(s_le[i], val_e), (masked(s_ll[i], pos_l, late * span + within), val_l)]
        )
        out[i] = with_levels(rows_of(out_e, out_l), rows_of(level_e, level_l))


def mix(parts, size, kv_local):
    starts = chunks_of(size)
    subsets = parts.shape[0] // kv_local
    shares = [[None] * len(starts) for _ in range(parts.shape[0])]
    for kv in range(kv_local):
        members = [j * kv_local + kv for j in range(subsets)]
        stats = [parts[s, size:, :].astype(F32) for s in members]
        for c in range(len(starts)):
            own = []
            for t in stats:
                level = t[PIECES * c : PIECES * c + 1]
                for piece in range(1, PIECES):
                    level = level + t[PIECES * c + piece : PIECES * c + piece + 1]
                own.append(level)
            peak = own[0]
            for level in own[1:]:
                peak = jnp.maximum(peak, level)
            weights = [jnp.exp2(level - peak) for level in own]
            total = weights[0]
            for w in weights[1:]:
                total = total + w
            for s, w in zip(members, weights):
                shares[s][c] = w / total
    flat = [w for share in shares for w in share]
    table = rows_of(*flat, jnp.zeros((HEAD_DIM - len(flat), HEAD_DIM), F32)).T
    results = []
    for kv in range(kv_local):
        mixed = 0.0
        for j in range(subsets):
            s = j * kv_local + kv
            pieces, done = [], 0
            for c, at in enumerate(starts):
                column = s * len(starts) + c
                pieces.append(table[done - at :, column : column + 1])
                done = at + HEAD_DIM
            mixed = mixed + rows_of(*pieces) * parts[s, :size, :].astype(F32)
        results.append(mixed)
    return results


def self_combine_kernel(order, parts, out):
    me = lax.axis_index("context")
    rows = out.shape[0]
    span = rows // 2
    swap = order[2 * me] > order[2 * me + 1]
    kv_local = out.shape[1] // (HEAD_DIM * GROUP)
    for kv, mixed in enumerate(mix(parts, GROUP * rows, kv_local)):
        for g in range(GROUP):
            head = kv * GROUP + g
            early = mixed[g * span : (g + 1) * span]
            late = mixed[(GROUP + g) * span : (GROUP + g + 1) * span]
            out[:, head * HEAD_DIM : (head + 1) * HEAD_DIM] = jnp.where(
                swap, rows_of(late, early), rows_of(early, late)
            ).astype(BF16)


def cross_combine_kernel(parts, out):
    rows = out.shape[0]
    kv_local = out.shape[1] // (HEAD_DIM * GROUP)
    for kv, mixed in enumerate(mix(parts, GROUP * rows, kv_local)):
        for g in range(GROUP):
            head = kv * GROUP + g
            out[:, head * HEAD_DIM : (head + 1) * HEAD_DIM] = mixed[
                g * rows : (g + 1) * rows
            ].astype(BF16)


def whole(memory=pltpu.VMEM):
    return pl.BlockSpec(memory_space=memory)


def attention(self_queries, self_keys, self_values, cross_queries, cross_keys, cross_values, span_order):
    context = lax.axis_size("context")
    rows = self_queries.shape[0]
    image = cross_keys.shape[0]
    heads = self_queries.shape[1] // HEAD_DIM
    height = context // RING
    patches = [
        [(z + a) * RING + x + b for a in range(PAIR) for b in range(HALF)]
        for z in range(0, height, PAIR)
        for x in range(0, RING, HALF)
    ]
    quads = [
        [z * RING + x + HALF * a + b for a in range(PAIR) for b in range(PAIR)]
        for z in range(height)
        for x in range(0, HALF, PAIR)
    ]
    columns = [
        [z * RING + x for z in range(p, height, PAIR)] for p in range(PAIR) for x in range(RING)
    ]
    key_devices = height * PAIR
    kv_rows = 2 * (rows + image)
    size = GROUP * rows

    queries, keys = pl.pallas_call(
        prepare_kernel,
        in_specs=[whole(pltpu.SMEM)] + [whole()] * 7,
        out_specs=[whole(), whole()],
        out_shape=[
            jax.ShapeDtypeStruct((RING, 2 * size, HEAD_DIM), BF16),
            jax.ShapeDtypeStruct((PAIR * PAIR, kv_rows, HEAD_DIM), BF16),
        ],
        name="prepare",
    )(
        span_order,
        jnp.asarray(frequencies()),
        self_queries,
        self_keys,
        self_values,
        cross_queries,
        cross_keys,
        cross_values,
    )
    keys = lax.all_to_all(keys, "context", 0, 0, axis_index_groups=quads)
    keys = lax.all_gather(keys, "context", axis_index_groups=columns)
    queries = lax.all_to_all(queries, "context", 0, 0, axis_index_groups=patches)
    keys = keys.reshape(key_devices, kv_rows, HEAD_DIM)

    out_rows = size + stat_rows(size)

    def attend(kernel, half, queries, order, kv_spec, scratch):
        return pl.pallas_call(
            lambda *refs: kernel(rows, *refs),
            grid=(RING // STEP,),
            in_specs=[whole(pltpu.SMEM)] * len(order)
            + [
                pl.BlockSpec((STEP, size, HEAD_DIM), lambda i: (i, half, 0)),
                kv_spec,
            ],
            out_specs=pl.BlockSpec((STEP, out_rows, HEAD_DIM), lambda i: (i, 0, 0)),
            out_shape=jax.ShapeDtypeStruct((RING, out_rows, HEAD_DIM), BF16),
            scratch_shapes=scratch,
            compiler_params=pltpu.CompilerParams(
                dimension_semantics=("arbitrary",), vmem_limit_bytes=48 * 1024 * 1024
            ),
            cost_estimate=pl.CostEstimate(
                flops=4 * RING * size * HEAD_DIM * key_devices * rows,
                transcendentals=RING * size * key_devices * rows,
                bytes_accessed=2 * key_devices * kv_rows * HEAD_DIM,
            ),
        )(*order, queries, keys)

    span_keys = key_devices * rows // 2
    image_keys = key_devices * image
    cross_parts = attend(
        cross_kernel,
        1,
        queries,
        (),
        whole(pl.ANY),
        [pltpu.VMEM((key_devices, 2 * image, HEAD_DIM), BF16)]
        + [pltpu.VMEM((image_keys, HEAD_DIM), BF16)] * 2
        + [pltpu.SemaphoreType.DMA],
    )
    cross_parts = lax.all_to_all(cross_parts, "context", 0, 0, axis_index_groups=patches)
    self_parts = attend(
        self_kernel,
        0,
        queries,
        (span_order,),
        pl.BlockSpec((key_devices, kv_rows, HEAD_DIM), lambda i: (0, 0, 0)),
        [pltpu.VMEM((span_keys, HEAD_DIM), BF16)] * 4 + [pltpu.VMEM((1, span_keys), jnp.int32)] * 2,
    )
    self_parts = lax.all_to_all(self_parts, "context", 0, 0, axis_index_groups=patches)
    out_shape = jax.ShapeDtypeStruct((rows, heads * HEAD_DIM), BF16)
    cross_out = pl.pallas_call(
        cross_combine_kernel,
        in_specs=[whole()],
        out_specs=whole(),
        out_shape=out_shape,
        name="cross_combine",
    )(cross_parts)
    self_out = pl.pallas_call(
        self_combine_kernel,
        in_specs=[whole(pltpu.SMEM), whole()],
        out_specs=whole(),
        out_shape=out_shape,
        name="self_combine",
    )(span_order, self_parts)
    return self_out, cross_out


def solution(mesh):
    rows = P(("groups", "context"), "tensor")
    return jax.shard_map(
        attention,
        mesh=mesh,
        in_specs=(rows,) * 6 + (P("groups"),),
        out_specs=(rows, rows),
        check_vma=False,
    )
```

```python
import jax
import jax.numpy as jnp
import numpy as np
from jax import lax
from jax.experimental import pallas as pl
from jax.experimental.pallas import tpu as pltpu
from jax.sharding import PartitionSpec as P


HEAD_DIM = 128
HEADS = 16
KV_HEADS = 4
GROUP = HEADS // KV_HEADS
RING = 8
PAIR = 2
COPIES = 8
STEP = 4
LEVEL_ROWS = 8
NEG_FILL = -1e30
LOG2E = 1.4426950408889634

BF16 = jnp.bfloat16
F32 = jnp.float32


def rows_of(*pieces):
    return jnp.concatenate(pieces, 0)


def frequencies():
    lane = np.arange(HEAD_DIM) % (HEAD_DIM // 2)
    return (500000.0 ** (-(lane * 2.0) / HEAD_DIM)).astype(np.float32)[None, :]


def spans_of(order, device):
    first, second = order[2 * device], order[2 * device + 1]
    return jnp.minimum(first, second), jnp.maximum(first, second)


def local_order(order, freq, rows):
    me = lax.axis_index("context")
    span = rows // 2
    swap = order[2 * me] > order[2 * me + 1]
    early, late = spans_of(order, me)
    row = lax.broadcasted_iota(jnp.int32, (rows, HEAD_DIM), 0)
    lane = lax.broadcasted_iota(jnp.int32, (rows, HEAD_DIM), 1)
    place = jnp.where(row < span, early * span + row, late * span + row - span)
    angle = place.astype(F32) * freq[...]
    cosine = jnp.cos(angle)
    sine = jnp.sin(angle)
    sine = jnp.where(lane < HEAD_DIM // 2, -sine, sine)

    def ordered(ref, head):
        x = plain(ref, head)
        return jnp.where(swap, rows_of(x[span:], x[:span]), x)

    def rotated(ref, head):
        x = ordered(ref, head)
        return x * cosine + pltpu.roll(x, HEAD_DIM // 2, 1) * sine

    return ordered, rotated


def plain(ref, head):
    return ref[:, head * HEAD_DIM : (head + 1) * HEAD_DIM].astype(F32)


def prepare_kernel(order, freq, sq, sk, sv, cq, ck, cv, q_out, kv_out):
    rows = sq.shape[0]
    span = rows // 2
    ordered, rotated = local_order(order, freq, rows)
    kv_local = sk.shape[1] // HEAD_DIM
    for kv in range(kv_local):
        block = rows_of(
            rotated(sk, kv), ordered(sv, kv), plain(ck, kv), plain(cv, kv)
        ).astype(BF16)
        for m in range(kv, kv_out.shape[0], kv_local):
            kv_out[m] = block
    for kv in range(kv_local):
        heads = range(kv * GROUP, (kv + 1) * GROUP)
        turned = [rotated(sq, head) for head in heads]
        block = rows_of(
            *[x[:span] for x in turned],
            *[x[span:] for x in turned],
            *[plain(cq, head) for head in heads],
        ).astype(BF16)
        for m in range(kv, q_out.shape[0], kv_local):
            q_out[m] = block


def scores(q, key):
    return lax.dot_general(q, key[...], (((1,), (1,)), ((), ())), preferred_element_type=F32)


def peak_of(parts):
    peak = parts[0].max(-1, keepdims=True)
    for s in parts[1:]:
        peak = jnp.maximum(peak, s.max(-1, keepdims=True))
    return jnp.maximum(peak, 0.1 * NEG_FILL)


def finish(parts):
    scale = HEAD_DIM ** (-0.5) * LOG2E
    shift = peak_of([s for s, _ in parts])
    total, mixed = 0.0, 0.0
    for s, val in parts:
        w = jnp.exp2((s - shift) * scale)
        total = total + w.sum(-1, keepdims=True)
        mixed = mixed + jnp.dot(w.astype(BF16), val[...], preferred_element_type=F32)
    some = total > 0.0
    safe = jnp.where(some, total, 1.0)
    level = jnp.where(some, shift * scale + jnp.log2(safe), NEG_FILL)
    return mixed * (1.0 / safe), level


def with_levels(mixed, level):
    half = HEAD_DIM // 2
    columns, ends = [], level.shape[0] // HEAD_DIM * HEAD_DIM
    for at in range(0, ends, HEAD_DIM):
        columns += parts_of(level[at : at + HEAD_DIM])
    first, second, third = parts_of(level[ends:])
    columns += [rows_of(first, second), rows_of(third, jnp.zeros((half, 1), F32))]
    lane = lax.broadcasted_iota(jnp.int32, (HEAD_DIM, HEAD_DIM), 1)
    table = jnp.zeros((HEAD_DIM, HEAD_DIM), F32)
    for c, column in enumerate(columns):
        table = jnp.where(lane == c, column, table)
    return rows_of(mixed, table.T[:LEVEL_ROWS]).astype(BF16)


def parts_of(level):
    parts = []
    for _ in range(3):
        part = level.astype(BF16).astype(F32)
        parts.append(part)
        level = level - part
    return parts


def levels_of(rows):
    whole_rows = [rows[c : c + 1] + rows[c + 1 : c + 2] + rows[c + 2 : c + 3] for c in (0, 3)]
    return whole_rows + [rows[6:7] + pltpu.roll(rows[6:7], HEAD_DIM // 2, 1) + rows[7:8]]


def gathered_rows(kv_hbm, low, kv_in, sems, targets):
    chunk = kv_in.shape[0] // sems.shape[0]
    rows = pl.ds(low, kv_in.shape[1])
    copies = [
        pltpu.make_async_copy(
            kv_hbm.at[pl.ds(c * chunk, chunk), rows, :], kv_in.at[pl.ds(c * chunk, chunk)], sems.at[c]
        )
        for c in range(sems.shape[0])
    ]
    for copy in copies:
        copy.start()

    def pair(i, carry):
        a = kv_in[2 * i].astype(F32)
        b = kv_in[2 * i + 1].astype(F32)
        for ref, lo, hi in targets:
            size = 2 * (hi - lo)
            at = pl.multiple_of(i * size, size)
            ref[pl.ds(at, size), :] = rows_of(a[lo:hi], b[lo:hi]).astype(BF16)
        return carry

    for c, copy in enumerate(copies):
        copy.wait()
        lax.fori_loop(c * chunk // 2, (c + 1) * chunk // 2, pair, 0)


def cross_kernel(rows, q_in, kv_hbm, out, kv_in, key, val, sems):
    image = kv_in.shape[1] // 2

    @pl.when(pl.program_id(0) == 0)
    def _():
        targets = [(key, 0, image), (val, image, 2 * image)]
        gathered_rows(kv_hbm, 2 * rows, kv_in, sems, targets)

    s = [scores(q_in[i], key) for i in range(STEP)]
    for i in range(STEP):
        out[i] = with_levels(*finish([(s[i], val)]))


def self_kernel(
    rows, order, q_in, kv_hbm, out, kv_in, key_e, key_l, val_e, val_l, pos_e, pos_l, sems
):
    step = pl.program_id(0)
    me = lax.axis_index("context")
    line, column = me // RING, me % RING
    span = rows // 2

    @pl.when(step == 0)
    def _():
        gathered_rows(
            kv_hbm,
            0,
            kv_in,
            sems,
            [
                (key_e, 0, span),
                (key_l, span, rows),
                (val_e, rows, rows + span),
                (val_l, rows + span, 2 * rows),
            ],
        )
        low = column // PAIR * PAIR
        lane = lax.broadcasted_iota(jnp.int32, pos_e.shape, 1)
        place_e, place_l = lane, lane
        for d in range(kv_in.shape[0]):
            early, late = spans_of(order, d // PAIR * RING + low + d % PAIR)
            here = lane >= d * span
            place_e = jnp.where(here, lane + (early - d) * span, place_e)
            place_l = jnp.where(here, lane + (late - d) * span, place_l)
        pos_e[...] = place_e
        pos_l[...] = place_l

    size = GROUP * span
    within = lax.broadcasted_iota(jnp.int32, (size, 1), 0) % span

    def masked(s, key_places, query_places):
        return jnp.where(key_places[...] <= query_places, s, NEG_FILL)

    s_ee, s_le, s_ll, ends = [], [], [], []
    for i in range(STEP):
        ends.append(spans_of(order, line * RING + step * STEP + i))
        q_e, q_l = q_in[i, :size], q_in[i, size:]
        s_ee.append(scores(q_e, key_e))
        s_le.append(scores(q_l, key_e))
        s_ll.append(scores(q_l, key_l))
    for i in range(STEP):
        early, late = ends[i]
        out_e, level_e = finish([(masked(s_ee[i], pos_e, early * span + within), val_e)])
        out_l, level_l = finish(
            [(s_le[i], val_e), (masked(s_ll[i], pos_l, late * span + within), val_l)]
        )
        out[i] = with_levels(rows_of(out_e, out_l), rows_of(level_e, level_l))


def mix(parts, size, kv_local):
    count = parts.shape[0]
    for kv in range(kv_local):
        members = range(kv, count, kv_local)
        levels = [levels_of(parts[s, size:, :].astype(F32)) for s in members]
        peak = levels[0]
        for level in levels[1:]:
            peak = [jnp.maximum(a, b) for a, b in zip(peak, level)]
        weights = [[jnp.exp2(a - b) for a, b in zip(level, peak)] for level in levels]
        total = weights[0]
        for weight in weights[1:]:
            total = [a + b for a, b in zip(total, weight)]
        flat = [a / b for weight in weights for a, b in zip(weight, total)]
        per = len(total)
        table = rows_of(*flat, jnp.zeros((HEAD_DIM - len(flat), HEAD_DIM), F32)).T
        mixed = 0.0
        for j, s in enumerate(members):
            share = rows_of(*[table[:, j * per + c : j * per + c + 1] for c in range(per)])[:size]
            mixed = mixed + share * parts[s, :size, :].astype(F32)
        yield mixed


def self_combine_kernel(order, parts, out):
    me = lax.axis_index("context")
    rows = out.shape[0]
    span = rows // 2
    swap = order[2 * me] > order[2 * me + 1]
    kv_local = out.shape[1] // (HEAD_DIM * GROUP)
    for kv, mixed in enumerate(mix(parts, GROUP * rows, kv_local)):
        for g in range(GROUP):
            head = kv * GROUP + g
            early = mixed[g * span : (g + 1) * span]
            late = mixed[(GROUP + g) * span : (GROUP + g + 1) * span]
            out[:, head * HEAD_DIM : (head + 1) * HEAD_DIM] = jnp.where(
                swap, rows_of(late, early), rows_of(early, late)
            ).astype(BF16)


def cross_combine_kernel(parts, out):
    rows = out.shape[0]
    kv_local = out.shape[1] // (HEAD_DIM * GROUP)
    for kv, mixed in enumerate(mix(parts, GROUP * rows, kv_local)):
        for g in range(GROUP):
            head = kv * GROUP + g
            out[:, head * HEAD_DIM : (head + 1) * HEAD_DIM] = mixed[
                g * rows : (g + 1) * rows
            ].astype(BF16)


def whole(memory=pltpu.VMEM):
    return pl.BlockSpec(memory_space=memory)


def attention(self_queries, self_keys, self_values, cross_queries, cross_keys, cross_values, span_order):
    context = lax.axis_size("context")
    rows = self_queries.shape[0]
    image = cross_keys.shape[0]
    heads = self_queries.shape[1] // HEAD_DIM
    height = context // RING
    lines = [[z * RING + x for x in range(RING)] for z in range(height)]
    squares = [
        [(z + a) * RING + x + b for a in range(PAIR) for b in range(PAIR)]
        for z in range(0, height, PAIR)
        for x in range(0, RING, PAIR)
    ]
    columns = [
        [z * RING + x for z in range(p, height, PAIR)] for p in range(PAIR) for x in range(RING)
    ]
    key_devices = height * PAIR
    kv_rows = 2 * (rows + image)
    size = GROUP * rows

    queries, keys = pl.pallas_call(
        prepare_kernel,
        in_specs=[whole(pltpu.SMEM)] + [whole()] * 7,
        out_specs=[whole(), whole()],
        out_shape=[
            jax.ShapeDtypeStruct((RING, 2 * size, HEAD_DIM), BF16),
            jax.ShapeDtypeStruct((PAIR * PAIR, kv_rows, HEAD_DIM), BF16),
        ],
        name="prepare",
    )(
        span_order,
        jnp.asarray(frequencies()),
        self_queries,
        self_keys,
        self_values,
        cross_queries,
        cross_keys,
        cross_values,
    )
    keys = lax.all_to_all(keys, "context", 0, 0, axis_index_groups=squares)
    keys = lax.all_gather(keys, "context", axis_index_groups=columns)
    queries = lax.all_to_all(queries, "context", 0, 0, axis_index_groups=lines)
    keys = keys.reshape(key_devices, kv_rows, HEAD_DIM)

    out_rows = size + LEVEL_ROWS

    def attend(kernel, half, queries, order, kv_spec, scratch):
        return pl.pallas_call(
            lambda *refs: kernel(rows, *refs),
            grid=(RING // STEP,),
            in_specs=[whole(pltpu.SMEM)] * len(order)
            + [
                pl.BlockSpec((STEP, size, HEAD_DIM), lambda i: (i, half, 0)),
                kv_spec,
            ],
            out_specs=pl.BlockSpec((STEP, out_rows, HEAD_DIM), lambda i: (i, 0, 0)),
            out_shape=jax.ShapeDtypeStruct((RING, out_rows, HEAD_DIM), BF16),
            scratch_shapes=scratch,
            compiler_params=pltpu.CompilerParams(
                dimension_semantics=("arbitrary",), vmem_limit_bytes=48 * 1024 * 1024
            ),
            cost_estimate=pl.CostEstimate(
                flops=4 * RING * size * HEAD_DIM * key_devices * rows,
                transcendentals=RING * size * key_devices * rows,
                bytes_accessed=2 * key_devices * kv_rows * HEAD_DIM,
            ),
        )(*order, queries, keys)

    span_keys = key_devices * rows // 2
    image_keys = key_devices * image
    cross_parts = attend(
        cross_kernel,
        1,
        queries,
        (),
        whole(pltpu.HBM),
        [pltpu.VMEM((key_devices, 2 * image, HEAD_DIM), BF16)]
        + [pltpu.VMEM((image_keys, HEAD_DIM), BF16)] * 2
        + [pltpu.SemaphoreType.DMA((COPIES,))],
    )
    cross_parts = lax.all_to_all(cross_parts, "context", 0, 0, axis_index_groups=lines)
    self_parts = attend(
        self_kernel,
        0,
        queries,
        (span_order,),
        whole(pltpu.HBM),
        [pltpu.VMEM((key_devices, 2 * rows, HEAD_DIM), BF16)]
        + [pltpu.VMEM((span_keys, HEAD_DIM), BF16)] * 4
        + [pltpu.VMEM((1, span_keys), jnp.int32)] * 2
        + [pltpu.SemaphoreType.DMA((COPIES,))],
    )
    self_parts = lax.all_to_all(self_parts, "context", 0, 0, axis_index_groups=lines)
    out_shape = jax.ShapeDtypeStruct((rows, heads * HEAD_DIM), BF16)
    small = pltpu.CompilerParams(vmem_limit_bytes=16 * 1024 * 1024)
    cross_out = pl.pallas_call(
        cross_combine_kernel,
        in_specs=[whole()],
        out_specs=whole(),
        out_shape=out_shape,
        compiler_params=small,
        name="cross_combine",
    )(cross_parts)
    self_out = pl.pallas_call(
        self_combine_kernel,
        in_specs=[whole(pltpu.SMEM), whole()],
        out_specs=whole(),
        out_shape=out_shape,
        compiler_params=small,
        name="self_combine",
    )(span_order, self_parts)
    return self_out, cross_out


def solution(mesh):
    rows = P(("groups", "context"), "tensor")
    return jax.shard_map(
        attention,
        mesh=mesh,
        in_specs=(rows,) * 6 + (P("groups"),),
        out_specs=(rows, rows),
        check_vma=False,
    )
```

```python
import jax
import jax.numpy as jnp
import numpy as np
from jax import lax
from jax.experimental import pallas as pl
from jax.experimental.pallas import tpu as pltpu
from jax.sharding import PartitionSpec as P


HEAD_DIM = 128
HEADS = 16
KV_HEADS = 4
GROUP = HEADS // KV_HEADS
RING = 8
PAIR = 2
STEP = 4
LEVEL_ROWS = 8
NEG_FILL = -1e30
LOG2E = 1.4426950408889634

BF16 = jnp.bfloat16
F32 = jnp.float32


def rows_of(*pieces):
    return jnp.concatenate(pieces, 0)


def frequencies():
    lane = np.arange(HEAD_DIM) % (HEAD_DIM // 2)
    return (500000.0 ** (-(lane * 2.0) / HEAD_DIM)).astype(np.float32)[None, :]


def spans_of(order, device):
    first, second = order[2 * device], order[2 * device + 1]
    return jnp.minimum(first, second), jnp.maximum(first, second)


def local_order(order, freq, rows):
    me = lax.axis_index("context")
    span = rows // 2
    swap = order[2 * me] > order[2 * me + 1]
    early, late = spans_of(order, me)
    row = lax.broadcasted_iota(jnp.int32, (rows, HEAD_DIM), 0)
    lane = lax.broadcasted_iota(jnp.int32, (rows, HEAD_DIM), 1)
    place = jnp.where(row < span, early * span + row, late * span + row - span)
    angle = place.astype(F32) * freq[...]
    cosine = jnp.cos(angle)
    sine = jnp.sin(angle)
    sine = jnp.where(lane < HEAD_DIM // 2, -sine, sine)

    def ordered(ref, head):
        x = plain(ref, head)
        return jnp.where(swap, rows_of(x[span:], x[:span]), x)

    def rotated(ref, head):
        x = ordered(ref, head)
        return x * cosine + pltpu.roll(x, HEAD_DIM // 2, 1) * sine

    return ordered, rotated


def plain(ref, head):
    return ref[:, head * HEAD_DIM : (head + 1) * HEAD_DIM].astype(F32)


def prepare_kernel(order, freq, sq, sk, sv, cq, ck, cv, q_out, kv_out):
    rows = sq.shape[0]
    span = rows // 2
    ordered, rotated = local_order(order, freq, rows)
    kv_local = sk.shape[1] // HEAD_DIM
    for kv in range(kv_local):
        block = rows_of(
            rotated(sk, kv), ordered(sv, kv), plain(ck, kv), plain(cv, kv)
        ).astype(BF16)
        for m in range(kv, kv_out.shape[0], kv_local):
            kv_out[m] = block
    for kv in range(kv_local):
        heads = range(kv * GROUP, (kv + 1) * GROUP)
        turned = [rotated(sq, head) for head in heads]
        block = rows_of(
            *[x[:span] for x in turned],
            *[x[span:] for x in turned],
            *[plain(cq, head) for head in heads],
        ).astype(BF16)
        for m in range(kv, q_out.shape[0], kv_local):
            q_out[m] = block


def scores(q, key):
    return lax.dot_general(q, key[...], (((1,), (1,)), ((), ())), preferred_element_type=F32)


def peak_of(parts):
    peak = parts[0].max(-1, keepdims=True)
    for s in parts[1:]:
        peak = jnp.maximum(peak, s.max(-1, keepdims=True))
    return jnp.maximum(peak, 0.1 * NEG_FILL)


def finish(parts):
    scale = HEAD_DIM ** (-0.5) * LOG2E
    shift = peak_of([s for s, _ in parts])
    total, mixed = 0.0, 0.0
    for s, val in parts:
        w = jnp.exp2((s - shift) * scale)
        total = total + w.sum(-1, keepdims=True)
        mixed = mixed + jnp.dot(w.astype(BF16), val[...], preferred_element_type=F32)
    some = total > 0.0
    safe = jnp.where(some, total, 1.0)
    level = jnp.where(some, shift * scale + jnp.log2(safe), NEG_FILL)
    return mixed * (1.0 / safe), level


def with_levels(mixed, level):
    half = HEAD_DIM // 2
    columns, ends = [], level.shape[0] // HEAD_DIM * HEAD_DIM
    for at in range(0, ends, HEAD_DIM):
        columns += parts_of(level[at : at + HEAD_DIM])
    first, second, third = parts_of(level[ends:])
    columns += [rows_of(first, second), rows_of(third, jnp.zeros((half, 1), F32))]
    lane = lax.broadcasted_iota(jnp.int32, (HEAD_DIM, HEAD_DIM), 1)
    table = jnp.zeros((HEAD_DIM, HEAD_DIM), F32)
    for c, column in enumerate(columns):
        table = jnp.where(lane == c, column, table)
    return rows_of(mixed, table.T[:LEVEL_ROWS]).astype(BF16)


def parts_of(level):
    parts = []
    for _ in range(3):
        part = level.astype(BF16).astype(F32)
        parts.append(part)
        level = level - part
    return parts


def levels_of(rows):
    whole_rows = [rows[c : c + 1] + rows[c + 1 : c + 2] + rows[c + 2 : c + 3] for c in (0, 3)]
    return whole_rows + [rows[6:7] + pltpu.roll(rows[6:7], HEAD_DIM // 2, 1) + rows[7:8]]


def sort_rows(kv_in, first, last, targets):
    def pair(i, carry):
        a = kv_in[2 * i].astype(F32)
        b = kv_in[2 * i + 1].astype(F32)
        for ref, lo, hi in targets:
            size = 2 * (hi - lo)
            at = pl.multiple_of(i * size, size)
            ref[pl.ds(at, size), :] = rows_of(a[lo:hi], b[lo:hi]).astype(BF16)
        return carry

    lax.fori_loop(first // 2, last // 2, pair, 0)


def cross_kernel(rows, q_in, kv_in, out, key, val):
    devices, image = kv_in.shape[0], kv_in.shape[1] // 2

    @pl.when(pl.program_id(0) == 0)
    def _():
        sort_rows(kv_in, 0, devices, [(key, 0, image), (val, image, 2 * image)])

    s = [scores(q_in[i], key) for i in range(STEP)]
    for i in range(STEP):
        out[i] = with_levels(*finish([(s[i], val)]))


def places_kernel(span, devices, order, pos_e, pos_l):
    low = lax.axis_index("context") % RING // PAIR * PAIR
    lane = lax.broadcasted_iota(jnp.int32, pos_e.shape, 1)
    place_e, place_l = lane, lane
    for d in range(devices):
        early, late = spans_of(order, d // PAIR * RING + low + d % PAIR)
        here = lane >= d * span
        place_e = jnp.where(here, lane + (early - d) * span, place_e)
        place_l = jnp.where(here, lane + (late - d) * span, place_l)
    pos_e[...] = place_e
    pos_l[...] = place_l


def self_kernel(
    rows, order, q_in, kv_in, pos_e, pos_l, out, key_e, key_l, val_e, val_l
):
    step = pl.program_id(0)
    me = lax.axis_index("context")
    line = me // RING
    span = rows // 2

    @pl.when(step == 0)
    def _():
        sort_rows(
            kv_in,
            0,
            kv_in.shape[0],
            [
                (key_e, 0, span),
                (key_l, span, rows),
                (val_e, rows, rows + span),
                (val_l, rows + span, 2 * rows),
            ],
        )

    size = GROUP * span
    within = lax.broadcasted_iota(jnp.int32, (size, 1), 0) % span

    def masked(s, key_places, query_places):
        return jnp.where(key_places[...] <= query_places, s, NEG_FILL)

    s_ee, s_le, s_ll, ends = [], [], [], []
    for i in range(STEP):
        ends.append(spans_of(order, line * RING + step * STEP + i))
        q_e, q_l = q_in[i, :size], q_in[i, size:]
        s_ee.append(scores(q_e, key_e))
        s_le.append(scores(q_l, key_e))
        s_ll.append(scores(q_l, key_l))
    for i in range(STEP):
        early, late = ends[i]
        out_e, level_e = finish([(masked(s_ee[i], pos_e, early * span + within), val_e)])
        out_l, level_l = finish(
            [(s_le[i], val_e), (masked(s_ll[i], pos_l, late * span + within), val_l)]
        )
        out[i] = with_levels(rows_of(out_e, out_l), rows_of(level_e, level_l))


def mix(parts, size, kv_local):
    count = parts.shape[0]
    for kv in range(kv_local):
        members = range(kv, count, kv_local)
        levels = [levels_of(parts[s, size:, :].astype(F32)) for s in members]
        peak = levels[0]
        for level in levels[1:]:
            peak = [jnp.maximum(a, b) for a, b in zip(peak, level)]
        weights = [[jnp.exp2(a - b) for a, b in zip(level, peak)] for level in levels]
        total = weights[0]
        for weight in weights[1:]:
            total = [a + b for a, b in zip(total, weight)]
        flat = [a / b for weight in weights for a, b in zip(weight, total)]
        per = len(total)
        table = rows_of(*flat, jnp.zeros((HEAD_DIM - len(flat), HEAD_DIM), F32)).T
        mixed = 0.0
        for j, s in enumerate(members):
            share = rows_of(*[table[:, j * per + c : j * per + c + 1] for c in range(per)])[:size]
            mixed = mixed + share * parts[s, :size, :].astype(F32)
        yield mixed


def self_combine_kernel(order, parts, out):
    me = lax.axis_index("context")
    rows = out.shape[0]
    span = rows // 2
    swap = order[2 * me] > order[2 * me + 1]
    kv_local = out.shape[1] // (HEAD_DIM * GROUP)
    for kv, mixed in enumerate(mix(parts, GROUP * rows, kv_local)):
        for g in range(GROUP):
            head = kv * GROUP + g
            early = mixed[g * span : (g + 1) * span]
            late = mixed[(GROUP + g) * span : (GROUP + g + 1) * span]
            out[:, head * HEAD_DIM : (head + 1) * HEAD_DIM] = jnp.where(
                swap, rows_of(late, early), rows_of(early, late)
            ).astype(BF16)


def cross_combine_kernel(parts, out):
    rows = out.shape[0]
    kv_local = out.shape[1] // (HEAD_DIM * GROUP)
    for kv, mixed in enumerate(mix(parts, GROUP * rows, kv_local)):
        for g in range(GROUP):
            head = kv * GROUP + g
            out[:, head * HEAD_DIM : (head + 1) * HEAD_DIM] = mixed[
                g * rows : (g + 1) * rows
            ].astype(BF16)


def whole(memory=pltpu.VMEM):
    return pl.BlockSpec(memory_space=memory)


def attention(self_queries, self_keys, self_values, cross_queries, cross_keys, cross_values, span_order):
    context = lax.axis_size("context")
    rows = self_queries.shape[0]
    image = cross_keys.shape[0]
    heads = self_queries.shape[1] // HEAD_DIM
    height = context // RING
    lines = [[z * RING + x for x in range(RING)] for z in range(height)]
    squares = [
        [(z + a) * RING + x + b for a in range(PAIR) for b in range(PAIR)]
        for z in range(0, height, PAIR)
        for x in range(0, RING, PAIR)
    ]
    columns = [
        [z * RING + x for z in range(p, height, PAIR)] for p in range(PAIR) for x in range(RING)
    ]
    key_devices = height * PAIR
    kv_rows = 2 * (rows + image)
    size = GROUP * rows

    queries, keys = pl.pallas_call(
        prepare_kernel,
        in_specs=[whole(pltpu.SMEM)] + [whole()] * 7,
        out_specs=[whole(), whole()],
        out_shape=[
            jax.ShapeDtypeStruct((RING, 2 * size, HEAD_DIM), BF16),
            jax.ShapeDtypeStruct((PAIR * PAIR, kv_rows, HEAD_DIM), BF16),
        ],
        name="prepare",
    )(
        span_order,
        jnp.asarray(frequencies()),
        self_queries,
        self_keys,
        self_values,
        cross_queries,
        cross_keys,
        cross_values,
    )
    keys = lax.all_to_all(keys, "context", 0, 0, axis_index_groups=squares)
    text, picture = keys[:, : 2 * rows, :], keys[:, 2 * rows :, :]
    text = lax.all_gather(text, "context", axis_index_groups=columns)
    far = height // PAIR // 2
    while far:
        ring = [
            (z * RING + x, (z + far * PAIR) % height * RING + x)
            for z in range(height)
            for x in range(RING)
        ]
        more = lax.ppermute(picture, "context", ring)
        picture = jnp.concatenate([picture, more], 0)
        far = far // 2
    queries = lax.all_to_all(queries, "context", 0, 0, axis_index_groups=lines)
    text = text.reshape(key_devices, 2 * rows, HEAD_DIM)
    picture = picture.reshape(key_devices, 2 * image, HEAD_DIM)

    span_keys = key_devices * rows // 2
    image_keys = key_devices * image
    places = pl.pallas_call(
        lambda *refs: places_kernel(rows // 2, key_devices, *refs),
        in_specs=[whole(pltpu.SMEM)],
        out_specs=[whole(), whole()],
        out_shape=[jax.ShapeDtypeStruct((1, span_keys), jnp.int32)] * 2,
        name="places",
    )(span_order)
    out_rows = size + LEVEL_ROWS

    def attend(kernel, half, keys, order, places, scratch):
        return pl.pallas_call(
            lambda *refs: kernel(rows, *refs),
            grid=(RING // STEP,),
            in_specs=[whole(pltpu.SMEM)] * len(order)
            + [
                pl.BlockSpec((STEP, size, HEAD_DIM), lambda i: (i, half, 0)),
                pl.BlockSpec(keys.shape, lambda i: (0, 0, 0)),
            ]
            + [pl.BlockSpec(p.shape, lambda i: (0, 0)) for p in places],
            out_specs=pl.BlockSpec((STEP, out_rows, HEAD_DIM), lambda i: (i, 0, 0)),
            out_shape=jax.ShapeDtypeStruct((RING, out_rows, HEAD_DIM), BF16),
            scratch_shapes=scratch,
            compiler_params=pltpu.CompilerParams(
                dimension_semantics=("arbitrary",), vmem_limit_bytes=48 * 1024 * 1024
            ),
            cost_estimate=pl.CostEstimate(
                flops=4 * RING * size * HEAD_DIM * key_devices * rows,
                transcendentals=RING * size * key_devices * rows,
                bytes_accessed=2 * key_devices * kv_rows * HEAD_DIM,
            ),
        )(*order, queries, keys, *places)

    cross_parts = attend(
        cross_kernel, 1, picture, (), (), [pltpu.VMEM((image_keys, HEAD_DIM), BF16)] * 2
    )
    cross_parts = lax.all_to_all(cross_parts, "context", 0, 0, axis_index_groups=lines)
    self_parts = attend(
        self_kernel, 0, text, (span_order,), places, [pltpu.VMEM((span_keys, HEAD_DIM), BF16)] * 4
    )
    self_parts = lax.all_to_all(self_parts, "context", 0, 0, axis_index_groups=lines)
    out_shape = jax.ShapeDtypeStruct((rows, heads * HEAD_DIM), BF16)
    small = pltpu.CompilerParams(vmem_limit_bytes=16 * 1024 * 1024)
    cross_out = pl.pallas_call(
        cross_combine_kernel,
        in_specs=[whole()],
        out_specs=whole(),
        out_shape=out_shape,
        compiler_params=small,
        name="cross_combine",
    )(cross_parts)
    self_out = pl.pallas_call(
        self_combine_kernel,
        in_specs=[whole(pltpu.SMEM), whole()],
        out_specs=whole(),
        out_shape=out_shape,
        compiler_params=small,
        name="self_combine",
    )(span_order, self_parts)
    return self_out, cross_out


def solution(mesh):
    rows = P(("groups", "context"), "tensor")
    return jax.shard_map(
        attention,
        mesh=mesh,
        in_specs=(rows,) * 6 + (P("groups"),),
        out_specs=(rows, rows),
        check_vma=False,
    )
```

```python
import jax
import jax.numpy as jnp
import numpy as np
from jax import lax
from jax.experimental import pallas as pl
from jax.experimental.pallas import tpu as pltpu
from jax.sharding import PartitionSpec as P


HEAD_DIM = 128
HEADS = 16
KV_HEADS = 4
GROUP = HEADS // KV_HEADS
RING = 8
PAIR = 2
STEP = 4
LEVEL_ROWS = 8
NEG_FILL = -1e30
LOG2E = 1.4426950408889634

BF16 = jnp.bfloat16
F32 = jnp.float32


def rows_of(*pieces):
    return jnp.concatenate(pieces, 0)


def frequencies():
    lane = np.arange(HEAD_DIM) % (HEAD_DIM // 2)
    return (500000.0 ** (-(lane * 2.0) / HEAD_DIM)).astype(np.float32)[None, :]


def spans_of(order, device):
    first, second = order[2 * device], order[2 * device + 1]
    return jnp.minimum(first, second), jnp.maximum(first, second)


def local_order(order, freq, rows):
    me = lax.axis_index("context")
    span = rows // 2
    swap = order[2 * me] > order[2 * me + 1]
    early, late = spans_of(order, me)
    row = lax.broadcasted_iota(jnp.int32, (rows, HEAD_DIM), 0)
    lane = lax.broadcasted_iota(jnp.int32, (rows, HEAD_DIM), 1)
    place = jnp.where(row < span, early * span + row, late * span + row - span)
    angle = place.astype(F32) * freq[...]
    cosine = jnp.cos(angle)
    sine = jnp.sin(angle)
    sine = jnp.where(lane < HEAD_DIM // 2, -sine, sine)

    def ordered(ref, head):
        x = plain(ref, head)
        return jnp.where(swap, rows_of(x[span:], x[:span]), x)

    def rotated(ref, head):
        x = ordered(ref, head)
        return x * cosine + pltpu.roll(x, HEAD_DIM // 2, 1) * sine

    return ordered, rotated


def plain(ref, head):
    return ref[:, head * HEAD_DIM : (head + 1) * HEAD_DIM].astype(F32)


def prepare_kernel(order, freq, sq, sk, sv, cq, ck, cv, q_out, kv_out):
    rows = sq.shape[0]
    span = rows // 2
    ordered, rotated = local_order(order, freq, rows)
    kv_local = sk.shape[1] // HEAD_DIM
    for kv in range(kv_local):
        block = rows_of(
            rotated(sk, kv), ordered(sv, kv), plain(ck, kv), plain(cv, kv)
        ).astype(BF16)
        for m in range(kv, kv_out.shape[0], kv_local):
            kv_out[m] = block
    for kv in range(kv_local):
        heads = range(kv * GROUP, (kv + 1) * GROUP)
        turned = [rotated(sq, head) for head in heads]
        block = rows_of(
            *[x[:span] for x in turned],
            *[x[span:] for x in turned],
            *[plain(cq, head) for head in heads],
        ).astype(BF16)
        for m in range(kv, q_out.shape[0], kv_local):
            q_out[m] = block


def scores(q, key):
    return lax.dot_general(q, key[...], (((1,), (1,)), ((), ())), preferred_element_type=F32)


def peak_of(parts):
    peak = parts[0].max(-1, keepdims=True)
    for s in parts[1:]:
        peak = jnp.maximum(peak, s.max(-1, keepdims=True))
    return jnp.maximum(peak, 0.1 * NEG_FILL)


def finish(parts):
    scale = HEAD_DIM ** (-0.5) * LOG2E
    shift = peak_of([s for s, _ in parts])
    total, mixed = 0.0, 0.0
    for s, val in parts:
        w = jnp.exp2((s - shift) * scale)
        total = total + w.sum(-1, keepdims=True)
        mixed = mixed + jnp.dot(w.astype(BF16), val[...], preferred_element_type=F32)
    some = total > 0.0
    safe = jnp.where(some, total, 1.0)
    level = jnp.where(some, shift * scale + jnp.log2(safe), NEG_FILL)
    return mixed * (1.0 / safe), level


def with_levels(mixed, level):
    half = HEAD_DIM // 2
    columns, ends = [], level.shape[0] // HEAD_DIM * HEAD_DIM
    for at in range(0, ends, HEAD_DIM):
        columns += parts_of(level[at : at + HEAD_DIM])
    first, second, third = parts_of(level[ends:])
    columns += [rows_of(first, second), rows_of(third, jnp.zeros((half, 1), F32))]
    lane = lax.broadcasted_iota(jnp.int32, (HEAD_DIM, HEAD_DIM), 1)
    table = jnp.zeros((HEAD_DIM, HEAD_DIM), F32)
    for c, column in enumerate(columns):
        table = jnp.where(lane == c, column, table)
    return rows_of(mixed, table.T[:LEVEL_ROWS]).astype(BF16)


def parts_of(level):
    parts = []
    for _ in range(3):
        part = level.astype(BF16).astype(F32)
        parts.append(part)
        level = level - part
    return parts


def levels_of(rows):
    whole_rows = [rows[c : c + 1] + rows[c + 1 : c + 2] + rows[c + 2 : c + 3] for c in (0, 3)]
    return whole_rows + [rows[6:7] + pltpu.roll(rows[6:7], HEAD_DIM // 2, 1) + rows[7:8]]


def sort_rows(kv_in, first, last, targets):
    def pair(i, carry):
        a = kv_in[2 * i].astype(F32)
        b = kv_in[2 * i + 1].astype(F32)
        for ref, lo, hi in targets:
            size = 2 * (hi - lo)
            at = pl.multiple_of(i * size, size)
            ref[pl.ds(at, size), :] = rows_of(a[lo:hi], b[lo:hi]).astype(BF16)
        return carry

    lax.fori_loop(first // 2, last // 2, pair, 0)


def cross_kernel(value_slots, rows, q_in, key_in, val_in, out, key, val):
    devices, image = key_in.shape[:2]

    @pl.when(pl.program_id(0) == 0)
    def _():
        sort_rows(key_in, 0, devices, [(key, 0, image)])
        for d in range(0, devices, 2):
            pair = [val_in[value_slots[i]].astype(F32) for i in (d, d + 1)]
            val[d * image : (d + 2) * image, :] = rows_of(*pair).astype(BF16)

    s = [scores(q_in[i], key) for i in range(STEP)]
    for i in range(STEP):
        out[i] = with_levels(*finish([(s[i], val)]))


def places_kernel(span, devices, order, pos_e, pos_l):
    low = lax.axis_index("context") % RING // PAIR * PAIR
    lane = lax.broadcasted_iota(jnp.int32, pos_e.shape, 1)
    place_e, place_l = lane, lane
    for d in range(devices):
        early, late = spans_of(order, d // PAIR * RING + low + d % PAIR)
        here = lane >= d * span
        place_e = jnp.where(here, lane + (early - d) * span, place_e)
        place_l = jnp.where(here, lane + (late - d) * span, place_l)
    pos_e[...] = place_e
    pos_l[...] = place_l


def self_kernel(
    rows, order, q_in, kv_in, pos_e, pos_l, out, key_e, key_l, val_e, val_l
):
    step = pl.program_id(0)
    me = lax.axis_index("context")
    line = me // RING
    span = rows // 2

    @pl.when(step == 0)
    def _():
        sort_rows(
            kv_in,
            0,
            kv_in.shape[0],
            [
                (key_e, 0, span),
                (key_l, span, rows),
                (val_e, rows, rows + span),
                (val_l, rows + span, 2 * rows),
            ],
        )

    size = GROUP * span
    within = lax.broadcasted_iota(jnp.int32, (size, 1), 0) % span

    def masked(s, key_places, query_places):
        return jnp.where(key_places[...] <= query_places, s, NEG_FILL)

    s_ee, s_le, s_ll, ends = [], [], [], []
    for i in range(STEP):
        ends.append(spans_of(order, line * RING + step * STEP + i))
        q_e, q_l = q_in[i, :size], q_in[i, size:]
        s_ee.append(scores(q_e, key_e))
        s_le.append(scores(q_l, key_e))
        s_ll.append(scores(q_l, key_l))
    for i in range(STEP):
        early, late = ends[i]
        out_e, level_e = finish([(masked(s_ee[i], pos_e, early * span + within), val_e)])
        out_l, level_l = finish(
            [(s_le[i], val_e), (masked(s_ll[i], pos_l, late * span + within), val_l)]
        )
        out[i] = with_levels(rows_of(out_e, out_l), rows_of(level_e, level_l))


def mix(parts, size, kv_local):
    count = parts.shape[0]
    for kv in range(kv_local):
        members = range(kv, count, kv_local)
        levels = [levels_of(parts[s, size:, :].astype(F32)) for s in members]
        peak = levels[0]
        for level in levels[1:]:
            peak = [jnp.maximum(a, b) for a, b in zip(peak, level)]
        weights = [[jnp.exp2(a - b) for a, b in zip(level, peak)] for level in levels]
        total = weights[0]
        for weight in weights[1:]:
            total = [a + b for a, b in zip(total, weight)]
        flat = [a / b for weight in weights for a, b in zip(weight, total)]
        per = len(total)
        table = rows_of(*flat, jnp.zeros((HEAD_DIM - len(flat), HEAD_DIM), F32)).T
        mixed = 0.0
        for j, s in enumerate(members):
            share = rows_of(*[table[:, j * per + c : j * per + c + 1] for c in range(per)])[:size]
            mixed = mixed + share * parts[s, :size, :].astype(F32)
        yield mixed


def self_combine_kernel(order, parts, out):
    me = lax.axis_index("context")
    rows = out.shape[0]
    span = rows // 2
    swap = order[2 * me] > order[2 * me + 1]
    kv_local = out.shape[1] // (HEAD_DIM * GROUP)
    for kv, mixed in enumerate(mix(parts, GROUP * rows, kv_local)):
        for g in range(GROUP):
            head = kv * GROUP + g
            early = mixed[g * span : (g + 1) * span]
            late = mixed[(GROUP + g) * span : (GROUP + g + 1) * span]
            out[:, head * HEAD_DIM : (head + 1) * HEAD_DIM] = jnp.where(
                swap, rows_of(late, early), rows_of(early, late)
            ).astype(BF16)


def cross_combine_kernel(parts, out):
    rows = out.shape[0]
    kv_local = out.shape[1] // (HEAD_DIM * GROUP)
    for kv, mixed in enumerate(mix(parts, GROUP * rows, kv_local)):
        for g in range(GROUP):
            head = kv * GROUP + g
            out[:, head * HEAD_DIM : (head + 1) * HEAD_DIM] = mixed[
                g * rows : (g + 1) * rows
            ].astype(BF16)


def whole(memory=pltpu.VMEM):
    return pl.BlockSpec(memory_space=memory)


def attention(self_queries, self_keys, self_values, cross_queries, cross_keys, cross_values, span_order):
    context = lax.axis_size("context")
    rows = self_queries.shape[0]
    image = cross_keys.shape[0]
    heads = self_queries.shape[1] // HEAD_DIM
    height = context // RING
    lines = [[z * RING + x for x in range(RING)] for z in range(height)]
    squares = [
        [(z + a) * RING + x + b for a in range(PAIR) for b in range(PAIR)]
        for z in range(0, height, PAIR)
        for x in range(0, RING, PAIR)
    ]
    columns = [
        [z * RING + x for z in range(p, height, PAIR)] for p in range(PAIR) for x in range(RING)
    ]
    key_devices = height * PAIR
    kv_rows = 2 * (rows + image)
    size = GROUP * rows

    queries, keys = pl.pallas_call(
        prepare_kernel,
        in_specs=[whole(pltpu.SMEM)] + [whole()] * 7,
        out_specs=[whole(), whole()],
        out_shape=[
            jax.ShapeDtypeStruct((RING, 2 * size, HEAD_DIM), BF16),
            jax.ShapeDtypeStruct((PAIR * PAIR, kv_rows, HEAD_DIM), BF16),
        ],
        name="prepare",
    )(
        span_order,
        jnp.asarray(frequencies()),
        self_queries,
        self_keys,
        self_values,
        cross_queries,
        cross_keys,
        cross_values,
    )
    keys = lax.all_to_all(keys, "context", 0, 0, axis_index_groups=squares)
    text, picture = keys[:, : 2 * rows, :], keys[:, 2 * rows :, :]
    text = lax.all_gather(text, "context", axis_index_groups=columns)
    turns = height // PAIR

    far = turns // 2
    picture = jnp.concatenate([picture, shifted(picture, far, height)], 0)
    picture_keys, picture_values = picture[:, :image, :], picture[:, image:, :]
    key_order = value_order = [0, -far % turns]
    far //= 2
    while far:
        more_keys = shifted(picture_keys, far, height)
        more_values = shifted(picture_values, -far, height)
        picture_keys = jnp.concatenate([picture_keys, more_keys], 0)
        picture_values = jnp.concatenate([picture_values, more_values], 0)
        key_order = key_order + [(o - far) % turns for o in key_order]
        value_order = value_order + [(o + far) % turns for o in value_order]
        far //= 2
    each = PAIR * PAIR
    value_slots = [value_order.index(o) * each + i for o in key_order for i in range(each)]
    queries = lax.all_to_all(queries, "context", 0, 0, axis_index_groups=lines)
    text = text.reshape(key_devices, 2 * rows, HEAD_DIM)

    span_keys = key_devices * rows // 2
    image_keys = key_devices * image
    places = pl.pallas_call(
        lambda *refs: places_kernel(rows // 2, key_devices, *refs),
        in_specs=[whole(pltpu.SMEM)],
        out_specs=[whole(), whole()],
        out_shape=[jax.ShapeDtypeStruct((1, span_keys), jnp.int32)] * 2,
        name="places",
    )(span_order)
    out_rows = size + LEVEL_ROWS

    def attend(kernel, half, order, keys, places, scratch):
        return pl.pallas_call(
            lambda *refs: kernel(rows, *refs),
            grid=(RING // STEP,),
            in_specs=[whole(pltpu.SMEM)] * len(order)
            + [
                pl.BlockSpec((STEP, size, HEAD_DIM), lambda i: (i, half, 0)),
            ]
            + [pl.BlockSpec(k.shape, lambda i: (0, 0, 0)) for k in keys]
            + [pl.BlockSpec(p.shape, lambda i: (0, 0)) for p in places],
            out_specs=pl.BlockSpec((STEP, out_rows, HEAD_DIM), lambda i: (i, 0, 0)),
            out_shape=jax.ShapeDtypeStruct((RING, out_rows, HEAD_DIM), BF16),
            scratch_shapes=scratch,
            compiler_params=pltpu.CompilerParams(
                dimension_semantics=("arbitrary",), vmem_limit_bytes=48 * 1024 * 1024
            ),
            cost_estimate=pl.CostEstimate(
                flops=4 * RING * size * HEAD_DIM * key_devices * rows,
                transcendentals=RING * size * key_devices * rows,
                bytes_accessed=2 * key_devices * kv_rows * HEAD_DIM,
            ),
        )(*order, queries, *keys, *places)

    cross_parts = attend(
        lambda *refs: cross_kernel(value_slots, *refs),
        1,
        (),
        (picture_keys, picture_values),
        (),
        [pltpu.VMEM((image_keys, HEAD_DIM), BF16)] * 2,
    )
    cross_parts = lax.all_to_all(cross_parts, "context", 0, 0, axis_index_groups=lines)
    self_parts = attend(
        self_kernel,
        0,
        (span_order,),
        (text,),
        places,
        [pltpu.VMEM((span_keys, HEAD_DIM), BF16)] * 4,
    )
    self_parts = lax.all_to_all(self_parts, "context", 0, 0, axis_index_groups=lines)
    out_shape = jax.ShapeDtypeStruct((rows, heads * HEAD_DIM), BF16)
    small = pltpu.CompilerParams(vmem_limit_bytes=16 * 1024 * 1024)
    cross_out = pl.pallas_call(
        cross_combine_kernel,
        in_specs=[whole()],
        out_specs=whole(),
        out_shape=out_shape,
        compiler_params=small,
        name="cross_combine",
    )(cross_parts)
    self_out = pl.pallas_call(
        self_combine_kernel,
        in_specs=[whole(pltpu.SMEM), whole()],
        out_specs=whole(),
        out_shape=out_shape,
        compiler_params=small,
        name="self_combine",
    )(span_order, self_parts)
    return self_out, cross_out


def shifted(x, far, height):
    ring = [
        (z * RING + c, (z + far * PAIR) % height * RING + c)
        for z in range(height)
        for c in range(RING)
    ]
    return lax.ppermute(x, "context", ring)


def solution(mesh):
    rows = P(("groups", "context"), "tensor")
    return jax.shard_map(
        attention,
        mesh=mesh,
        in_specs=(rows,) * 6 + (P("groups"),),
        out_specs=(rows, rows),
        check_vma=False,
    )
```

```python
import jax
import jax.numpy as jnp
import numpy as np
from jax import lax
from jax.experimental import pallas as pl
from jax.experimental.pallas import tpu as pltpu
from jax.sharding import PartitionSpec as P


HEAD_DIM = 128
HEADS = 16
KV_HEADS = 4
GROUP = HEADS // KV_HEADS
RING = 8
PAIR = 2
STEP = 4
LEVEL_ROWS = 8
NEG_FILL = -1e30
LOG2E = 1.4426950408889634

BF16 = jnp.bfloat16
F32 = jnp.float32


def rows_of(*pieces):
    return jnp.concatenate(pieces, 0)


def frequencies():
    lane = np.arange(HEAD_DIM) % (HEAD_DIM // 2)
    return (500000.0 ** (-(lane * 2.0) / HEAD_DIM)).astype(np.float32)[None, :]


def spans_of(order, device):
    first, second = order[2 * device], order[2 * device + 1]
    return jnp.minimum(first, second), jnp.maximum(first, second)


def local_order(order, freq, rows):
    me = lax.axis_index("context")
    span = rows // 2
    swap = order[2 * me] > order[2 * me + 1]
    early, late = spans_of(order, me)
    row = lax.broadcasted_iota(jnp.int32, (rows, HEAD_DIM), 0)
    lane = lax.broadcasted_iota(jnp.int32, (rows, HEAD_DIM), 1)
    place = jnp.where(row < span, early * span + row, late * span + row - span)
    angle = place.astype(F32) * freq[...]
    cosine = jnp.cos(angle)
    sine = jnp.sin(angle)
    sine = jnp.where(lane < HEAD_DIM // 2, -sine, sine)

    def ordered(ref, head):
        x = plain(ref, head)
        return jnp.where(swap, rows_of(x[span:], x[:span]), x)

    def rotated(ref, head):
        x = ordered(ref, head)
        return x * cosine + pltpu.roll(x, HEAD_DIM // 2, 1) * sine

    return ordered, rotated


def plain(ref, head):
    return ref[:, head * HEAD_DIM : (head + 1) * HEAD_DIM].astype(F32)


def key_kernel(order, freq, sk, sv, ck, cv, kv_out):
    ordered, rotated = local_order(order, freq, sk.shape[0])
    kv_local = sk.shape[1] // HEAD_DIM
    for kv in range(kv_local):
        block = rows_of(
            rotated(sk, kv), ordered(sv, kv), plain(ck, kv), plain(cv, kv)
        ).astype(BF16)
        for m in range(kv, kv_out.shape[0], kv_local):
            kv_out[m] = block


def query_kernel(order, freq, sq, cq, q_out):
    rows = sq.shape[0]
    span = rows // 2
    _, rotated = local_order(order, freq, rows)
    kv_local = sq.shape[1] // (HEAD_DIM * GROUP)
    for kv in range(kv_local):
        heads = range(kv * GROUP, (kv + 1) * GROUP)
        turned = [rotated(sq, head) for head in heads]
        block = rows_of(
            *[x[:span] for x in turned],
            *[x[span:] for x in turned],
            *[plain(cq, head) for head in heads],
        ).astype(BF16)
        for m in range(kv, q_out.shape[0], kv_local):
            q_out[m] = block


def scores(q, key):
    return lax.dot_general(q, key[...], (((1,), (1,)), ((), ())), preferred_element_type=F32)


def peak_of(parts):
    peak = parts[0].max(-1, keepdims=True)
    for s in parts[1:]:
        peak = jnp.maximum(peak, s.max(-1, keepdims=True))
    return jnp.maximum(peak, 0.1 * NEG_FILL)


def finish(parts):
    scale = HEAD_DIM ** (-0.5) * LOG2E
    shift = peak_of([s for s, _ in parts])
    total, mixed = 0.0, 0.0
    for s, val in parts:
        w = jnp.exp2((s - shift) * scale)
        total = total + w.sum(-1, keepdims=True)
        mixed = mixed + jnp.dot(w.astype(BF16), val[...], preferred_element_type=F32)
    some = total > 0.0
    safe = jnp.where(some, total, 1.0)
    level = jnp.where(some, shift * scale + jnp.log2(safe), NEG_FILL)
    return mixed * (1.0 / safe), level


def with_levels(mixed, level):
    half = HEAD_DIM // 2
    columns, ends = [], level.shape[0] // HEAD_DIM * HEAD_DIM
    for at in range(0, ends, HEAD_DIM):
        columns += parts_of(level[at : at + HEAD_DIM])
    first, second, third = parts_of(level[ends:])
    columns += [rows_of(first, second), rows_of(third, jnp.zeros((half, 1), F32))]
    lane = lax.broadcasted_iota(jnp.int32, (HEAD_DIM, HEAD_DIM), 1)
    table = jnp.zeros((HEAD_DIM, HEAD_DIM), F32)
    for c, column in enumerate(columns):
        table = jnp.where(lane == c, column, table)
    return rows_of(mixed, table.T[:LEVEL_ROWS]).astype(BF16)


def parts_of(level):
    parts = []
    for _ in range(3):
        part = level.astype(BF16).astype(F32)
        parts.append(part)
        level = level - part
    return parts


def levels_of(rows):
    whole_rows = [rows[c : c + 1] + rows[c + 1 : c + 2] + rows[c + 2 : c + 3] for c in (0, 3)]
    return whole_rows + [rows[6:7] + pltpu.roll(rows[6:7], HEAD_DIM // 2, 1) + rows[7:8]]


def sort_rows(kv_in, first, last, targets):
    def pair(i, carry):
        a = kv_in[2 * i].astype(F32)
        b = kv_in[2 * i + 1].astype(F32)
        for ref, lo, hi in targets:
            size = 2 * (hi - lo)
            at = pl.multiple_of(i * size, size)
            ref[pl.ds(at, size), :] = rows_of(a[lo:hi], b[lo:hi]).astype(BF16)
        return carry

    lax.fori_loop(first // 2, last // 2, pair, 0)


def cross_kernel(value_slots, rows, q_in, key_in, val_in, out, key, val):
    devices, image = key_in.shape[:2]

    @pl.when(pl.program_id(0) == 0)
    def _():
        sort_rows(key_in, 0, devices, [(key, 0, image)])
        for d in range(0, devices, 2):
            pair = [val_in[value_slots[i]].astype(F32) for i in (d, d + 1)]
            val[d * image : (d + 2) * image, :] = rows_of(*pair).astype(BF16)

    s = [scores(q_in[i], key) for i in range(STEP)]
    for i in range(STEP):
        out[i] = with_levels(*finish([(s[i], val)]))


def places_kernel(span, devices, order, pos_e, pos_l):
    low = lax.axis_index("context") % RING // PAIR * PAIR
    lane = lax.broadcasted_iota(jnp.int32, pos_e.shape, 1)
    place_e, place_l = lane, lane
    for d in range(devices):
        early, late = spans_of(order, d // PAIR * RING + low + d % PAIR)
        here = lane >= d * span
        place_e = jnp.where(here, lane + (early - d) * span, place_e)
        place_l = jnp.where(here, lane + (late - d) * span, place_l)
    pos_e[...] = place_e
    pos_l[...] = place_l


def self_kernel(
    rows, order, q_in, kv_in, pos_e, pos_l, out, key_e, key_l, val_e, val_l
):
    step = pl.program_id(0)
    me = lax.axis_index("context")
    line = me // RING
    span = rows // 2

    @pl.when(step == 0)
    def _():
        sort_rows(
            kv_in,
            0,
            kv_in.shape[0],
            [
                (key_e, 0, span),
                (key_l, span, rows),
                (val_e, rows, rows + span),
                (val_l, rows + span, 2 * rows),
            ],
        )

    size = GROUP * span
    within = lax.broadcasted_iota(jnp.int32, (size, 1), 0) % span

    def masked(s, key_places, query_places):
        return jnp.where(key_places[...] <= query_places, s, NEG_FILL)

    s_ee, s_le, s_ll, ends = [], [], [], []
    for i in range(STEP):
        ends.append(spans_of(order, line * RING + step * STEP + i))
        q_e, q_l = q_in[i, :size], q_in[i, size:]
        s_ee.append(scores(q_e, key_e))
        s_le.append(scores(q_l, key_e))
        s_ll.append(scores(q_l, key_l))
    for i in range(STEP):
        early, late = ends[i]
        out_e, level_e = finish([(masked(s_ee[i], pos_e, early * span + within), val_e)])
        out_l, level_l = finish(
            [(s_le[i], val_e), (masked(s_ll[i], pos_l, late * span + within), val_l)]
        )
        out[i] = with_levels(rows_of(out_e, out_l), rows_of(level_e, level_l))


def mix(parts, size, kv_local):
    count = parts.shape[0]
    for kv in range(kv_local):
        members = range(kv, count, kv_local)
        levels = [levels_of(parts[s, size:, :].astype(F32)) for s in members]
        peak = levels[0]
        for level in levels[1:]:
            peak = [jnp.maximum(a, b) for a, b in zip(peak, level)]
        weights = [[jnp.exp2(a - b) for a, b in zip(level, peak)] for level in levels]
        total = weights[0]
        for weight in weights[1:]:
            total = [a + b for a, b in zip(total, weight)]
        flat = [a / b for weight in weights for a, b in zip(weight, total)]
        per = len(total)
        table = rows_of(*flat, jnp.zeros((HEAD_DIM - len(flat), HEAD_DIM), F32)).T
        mixed = 0.0
        for j, s in enumerate(members):
            share = rows_of(*[table[:, j * per + c : j * per + c + 1] for c in range(per)])[:size]
            mixed = mixed + share * parts[s, :size, :].astype(F32)
        yield mixed


def self_combine_kernel(order, parts, out):
    me = lax.axis_index("context")
    rows = out.shape[0]
    span = rows // 2
    swap = order[2 * me] > order[2 * me + 1]
    kv_local = out.shape[1] // (HEAD_DIM * GROUP)
    for kv, mixed in enumerate(mix(parts, GROUP * rows, kv_local)):
        for g in range(GROUP):
            head = kv * GROUP + g
            early = mixed[g * span : (g + 1) * span]
            late = mixed[(GROUP + g) * span : (GROUP + g + 1) * span]
            out[:, head * HEAD_DIM : (head + 1) * HEAD_DIM] = jnp.where(
                swap, rows_of(late, early), rows_of(early, late)
            ).astype(BF16)


def cross_combine_kernel(parts, out):
    rows = out.shape[0]
    kv_local = out.shape[1] // (HEAD_DIM * GROUP)
    for kv, mixed in enumerate(mix(parts, GROUP * rows, kv_local)):
        for g in range(GROUP):
            head = kv * GROUP + g
            out[:, head * HEAD_DIM : (head + 1) * HEAD_DIM] = mixed[
                g * rows : (g + 1) * rows
            ].astype(BF16)


def whole(memory=pltpu.VMEM):
    return pl.BlockSpec(memory_space=memory)


def attention(self_queries, self_keys, self_values, cross_queries, cross_keys, cross_values, span_order):
    context = lax.axis_size("context")
    rows = self_queries.shape[0]
    image = cross_keys.shape[0]
    heads = self_queries.shape[1] // HEAD_DIM
    height = context // RING
    lines = [[z * RING + x for x in range(RING)] for z in range(height)]
    squares = [
        [(z + a) * RING + x + b for a in range(PAIR) for b in range(PAIR)]
        for z in range(0, height, PAIR)
        for x in range(0, RING, PAIR)
    ]
    columns = [
        [z * RING + x for z in range(p, height, PAIR)] for p in range(PAIR) for x in range(RING)
    ]
    key_devices = height * PAIR
    kv_rows = 2 * (rows + image)
    size = GROUP * rows

    freq = jnp.asarray(frequencies())
    keys = pl.pallas_call(
        key_kernel,
        in_specs=[whole(pltpu.SMEM)] + [whole()] * 5,
        out_specs=whole(),
        out_shape=jax.ShapeDtypeStruct((PAIR * PAIR, kv_rows, HEAD_DIM), BF16),
        name="keys",
    )(span_order, freq, self_keys, self_values, cross_keys, cross_values)
    keys = lax.all_to_all(keys, "context", 0, 0, axis_index_groups=squares)
    queries = pl.pallas_call(
        query_kernel,
        in_specs=[whole(pltpu.SMEM)] + [whole()] * 3,
        out_specs=whole(),
        out_shape=jax.ShapeDtypeStruct((RING, 2 * size, HEAD_DIM), BF16),
        name="queries",
    )(span_order, freq, self_queries, cross_queries)
    text, picture = keys[:, : 2 * rows, :], keys[:, 2 * rows :, :]
    text = lax.all_gather(text, "context", axis_index_groups=columns)
    turns = height // PAIR

    far = turns // 2
    picture = jnp.concatenate([picture, shifted(picture, far, height)], 0)
    picture_keys, picture_values = picture[:, :image, :], picture[:, image:, :]
    key_order = value_order = [0, -far % turns]
    far //= 2
    while far:
        more_keys = shifted(picture_keys, far, height)
        more_values = shifted(picture_values, -far, height)
        picture_keys = jnp.concatenate([picture_keys, more_keys], 0)
        picture_values = jnp.concatenate([picture_values, more_values], 0)
        key_order = key_order + [(o - far) % turns for o in key_order]
        value_order = value_order + [(o + far) % turns for o in value_order]
        far //= 2
    each = PAIR * PAIR
    value_slots = [value_order.index(o) * each + i for o in key_order for i in range(each)]
    queries = lax.all_to_all(queries, "context", 0, 0, axis_index_groups=lines)
    text = text.reshape(key_devices, 2 * rows, HEAD_DIM)

    span_keys = key_devices * rows // 2
    image_keys = key_devices * image
    places = pl.pallas_call(
        lambda *refs: places_kernel(rows // 2, key_devices, *refs),
        in_specs=[whole(pltpu.SMEM)],
        out_specs=[whole(), whole()],
        out_shape=[jax.ShapeDtypeStruct((1, span_keys), jnp.int32)] * 2,
        name="places",
    )(span_order)
    out_rows = size + LEVEL_ROWS

    def attend(kernel, half, order, keys, places, scratch):
        return pl.pallas_call(
            lambda *refs: kernel(rows, *refs),
            grid=(RING // STEP,),
            in_specs=[whole(pltpu.SMEM)] * len(order)
            + [
                pl.BlockSpec((STEP, size, HEAD_DIM), lambda i: (i, half, 0)),
            ]
            + [pl.BlockSpec(k.shape, lambda i: (0, 0, 0)) for k in keys]
            + [pl.BlockSpec(p.shape, lambda i: (0, 0)) for p in places],
            out_specs=pl.BlockSpec((STEP, out_rows, HEAD_DIM), lambda i: (i, 0, 0)),
            out_shape=jax.ShapeDtypeStruct((RING, out_rows, HEAD_DIM), BF16),
            scratch_shapes=scratch,
            compiler_params=pltpu.CompilerParams(
                dimension_semantics=("arbitrary",), vmem_limit_bytes=48 * 1024 * 1024
            ),
            cost_estimate=pl.CostEstimate(
                flops=4 * RING * size * HEAD_DIM * key_devices * rows,
                transcendentals=RING * size * key_devices * rows,
                bytes_accessed=2 * key_devices * kv_rows * HEAD_DIM,
            ),
        )(*order, queries, *keys, *places)

    cross_parts = attend(
        lambda *refs: cross_kernel(value_slots, *refs),
        1,
        (),
        (picture_keys, picture_values),
        (),
        [pltpu.VMEM((image_keys, HEAD_DIM), BF16)] * 2,
    )
    cross_parts = lax.all_to_all(cross_parts, "context", 0, 0, axis_index_groups=lines)
    self_parts = attend(
        self_kernel,
        0,
        (span_order,),
        (text,),
        places,
        [pltpu.VMEM((span_keys, HEAD_DIM), BF16)] * 4,
    )
    self_parts = lax.all_to_all(self_parts, "context", 0, 0, axis_index_groups=lines)
    out_shape = jax.ShapeDtypeStruct((rows, heads * HEAD_DIM), BF16)
    small = pltpu.CompilerParams(vmem_limit_bytes=16 * 1024 * 1024)
    cross_out = pl.pallas_call(
        cross_combine_kernel,
        in_specs=[whole()],
        out_specs=whole(),
        out_shape=out_shape,
        compiler_params=small,
        name="cross_combine",
    )(cross_parts)
    self_out = pl.pallas_call(
        self_combine_kernel,
        in_specs=[whole(pltpu.SMEM), whole()],
        out_specs=whole(),
        out_shape=out_shape,
        compiler_params=small,
        name="self_combine",
    )(span_order, self_parts)
    return self_out, cross_out


def shifted(x, far, height):
    ring = [
        (z * RING + c, (z + far * PAIR) % height * RING + c)
        for z in range(height)
        for c in range(RING)
    ]
    return lax.ppermute(x, "context", ring)


def solution(mesh):
    rows = P(("groups", "context"), "tensor")
    return jax.shard_map(
        attention,
        mesh=mesh,
        in_specs=(rows,) * 6 + (P("groups"),),
        out_specs=(rows, rows),
        check_vma=False,
    )
```
